32 devices in a mesh: data: 1 (over z), outer: 4 (over y), expert: 8 (over x, core).
Axes of the slice: x: 4, y: 4, z: 1, core: 2. Of those that a mesh axis runs over, the one named last changes fastest.
The devices are a block of a 4x4x8 slice.
Arguments:
- x_disp: bfloat16 [32, 128, 8, 2048], P('data', ('outer', 'expert'))
- w_gate: bfloat16 [128, 2048, 768], P(('outer', 'expert'))
- w_up: bfloat16 [128, 2048, 768], P(('outer', 'expert'))
- w_down: bfloat16 [128, 768, 2048], P(('outer', 'expert'))
- slot_idx: int32 [4096, 8], P(('data', 'outer', 'expert'))
- expert_ids: int32 [4096, 8], P(('data', 'outer', 'expert'))
- gate_wts: float32 [4096, 8], P(('data', 'outer', 'expert'))
Outputs:
- output: bfloat16 [4096, 2048], P(('data', 'outer', 'expert'))
All inputs are finite; a program needn't handle non-finite values.
Results may differ from the reference program's by a relative error of at most 0.00826245.
Values are sent between devices in bfloat16 or wider.
A program may use at most 768 MiB of HBM per device.

```python
import jax
import jax.numpy as jnp
from jax import lax

D = 2048
FF = 768
EXPERTS = 128
TOP = 8
CAP = 8
OUTER = 4
INNER = 8
NODE_MAX = 2
TOK = 128

GROUP_DEVS = OUTER * INNER
TOKENS = GROUP_DEVS * TOK
BLOCK_EXPERTS = EXPERTS // OUTER
BONUS = 2 ** 20


def draw_routing(key):
    key_hot, key_block, key_noise, key_bias = jax.random.split(key, 4)
    hot_expert = jax.random.randint(key_hot, (), 0, EXPERTS)
    forced = (jnp.arange(TOKENS) % TOK < CAP)[:, None]
    blocks = jnp.arange(OUTER)
    block_score = jax.random.randint(key_block, (TOKENS, OUTER), 0, 1024) * OUTER + blocks
    block_score = block_score + jnp.where(forced & (blocks == hot_expert // BLOCK_EXPERTS), BONUS, 0)
    best_blocks = jnp.argsort(-block_score, axis=1)[:, :NODE_MAX]
    chosen = jnp.any(best_blocks[:, :, None] == blocks[None, None, :], axis=1)
    experts = jnp.arange(EXPERTS)
    expert_bias = jax.random.randint(key_bias, (EXPERTS,), 0, 1024)
    rand_noise = jax.random.randint(key_noise, (TOKENS, EXPERTS), 0, 1024)
    expert_score = ((rand_noise + expert_bias) * EXPERTS + experts).reshape(TOKENS, OUTER, BLOCK_EXPERTS)
    block_best = expert_score == jnp.max(expert_score, axis=2, keepdims=True)
    expert_score = jnp.where(chosen[:, :, None], expert_score + jnp.where(block_best, BONUS, 0), -1)
    expert_score = expert_score.reshape(TOKENS, EXPERTS) + jnp.where(forced & (experts == hot_expert), 2 * BONUS, 0)
    expert_ids = jnp.sort(jnp.argsort(-expert_score, axis=1)[:, :TOP], axis=1)
    source = jnp.arange(TOKENS) // TOK
    group_id = (source[:, None] * EXPERTS + expert_ids).reshape(-1)
    sort_order = jnp.argsort(group_id, stable=True)
    counts = jnp.zeros(GROUP_DEVS * EXPERTS, jnp.int32).at[group_id].add(1)
    starts = jnp.cumsum(counts) - counts
    sorted_rank = jnp.arange(TOKENS * TOP) - starts[group_id[sort_order]]
    slot_rank = jnp.zeros(TOKENS * TOP, jnp.int32).at[sort_order].set(sorted_rank.astype(jnp.int32))
    slot_idx = jnp.where(slot_rank < CAP, slot_rank, -1).reshape(TOKENS, TOP)
    return slot_idx.astype(jnp.int32), expert_ids.astype(jnp.int32)


def setup_inputs(seed: int = 0, part: int = 0) -> dict:
    base_key = jax.random.key(seed)
    key_wg, key_wu, key_wd = jax.random.split(base_key, 3)
    part_key = jax.random.fold_in(base_key, part)
    key_x, key_route, key_gate = jax.random.split(part_key, 3)
    x_disp = jax.random.normal(key_x, (GROUP_DEVS, EXPERTS, CAP, D), jnp.float32).astype(jnp.bfloat16)
    w_gate = (jax.random.normal(key_wg, (EXPERTS, D, FF), jnp.float32) * D ** -0.5).astype(jnp.bfloat16)
    w_up = (jax.random.normal(key_wu, (EXPERTS, D, FF), jnp.float32) * D ** -0.5).astype(jnp.bfloat16)
    w_down = (jax.random.normal(key_wd, (EXPERTS, FF, D), jnp.float32) * FF ** -0.5).astype(jnp.bfloat16)
    slot_idx, expert_ids = draw_routing(key_route)
    gate_wts = jax.nn.softmax(1.5 * jax.random.normal(key_gate, (TOKENS, TOP), jnp.float32), axis=1)
    return {"x_disp": x_disp, "w_gate": w_gate, "w_up": w_up, "w_down": w_down, "slot_idx": slot_idx, "expert_ids": expert_ids, "gate_wts": gate_wts}


def expert_ffn(expert_args):
    rows_e, gate_e, up_e, down_e = expert_args
    gate_proj = jnp.dot(rows_e, gate_e, preferred_element_type=jnp.float32)
    up_proj = jnp.dot(rows_e, up_e, preferred_element_type=jnp.float32)
    hidden = (jax.nn.silu(gate_proj) * up_proj).astype(jnp.bfloat16)
    return jnp.dot(hidden, down_e, preferred_element_type=jnp.float32).astype(jnp.bfloat16)


def reference(x_disp, w_gate, w_up, w_down, slot_idx, expert_ids, gate_wts):
    x_rows = jnp.transpose(x_disp, (1, 0, 2, 3)).reshape(EXPERTS, GROUP_DEVS * CAP, D)
    y_out = lax.map(expert_ffn, (x_rows, w_gate, w_up, w_down))
    y_flat = y_out.reshape(EXPERTS * GROUP_DEVS * CAP, D)
    source = jnp.arange(TOKENS) // TOK
    kept_mask = slot_idx >= 0
    flat_idx = jnp.where(kept_mask, (expert_ids * GROUP_DEVS + source[:, None]) * CAP + slot_idx, 0)
    weight = jnp.where(kept_mask, gate_wts, 0.0)

    def combine(source_args):
        pick_idx, pick_wts = source_args
        picked = jnp.take(y_flat, pick_idx, axis=0).astype(jnp.float32)
        return jnp.sum(picked * pick_wts[:, :, None], axis=1).astype(jnp.bfloat16)

    combined = lax.map(combine, (flat_idx.reshape(GROUP_DEVS, TOK, TOP), weight.reshape(GROUP_DEVS, TOK, TOP)))
    return combined.reshape(TOKENS, D)
```

```python
import jax
import jax.numpy as jnp
from jax import lax
from jax.experimental import pallas as pl
from jax.experimental.pallas import tpu as pltpu
from jax.sharding import PartitionSpec as P

MESH_ID = pl.DeviceIdType.MESH
FF_CHUNK = 256
D_CHUNK = 512
BF16_MAX = 3.3895313892515355e38


def ring_distance(step, size):
    return min(step, size - step)


def peer_offsets(outer_devs, inner_devs):
    chips = inner_devs // 2
    steps = [(dy, dx, flip) for dx in range(chips) for dy in range(outer_devs) for flip in range(2)]
    steps = [s for s in steps if s != (0, 0, 0)]
    return sorted(steps, key=lambda s: -(ring_distance(s[0], outer_devs) + ring_distance(s[1], chips)))


def make_kernel(outer_devs, inner_devs, experts, capacity, width, ff, tokens, top):
    group = outer_devs * inner_devs
    rows = group * capacity
    chips = inner_devs // 2
    offsets = peer_offsets(outer_devs, inner_devs)
    n_ff, n_d = ff // FF_CHUNK, width // D_CHUNK

    def kernel(x_hbm, wg_hbm, wu_hbm, wd_hbm, slot_ref, eid_ref, gate_ref, out_ref,
               x_buf, wg_buf, wu_buf, wd_buf, h_buf, send_buf, recv_buf, acc, w_buf, used_buf,
               x_sem, g_sem, u_sem, d_sem, send_sem, recv_sem):
        row = lax.axis_index("outer")
        col = lax.axis_index("expert")
        me = row * inner_devs + col
        chip, core = col // 2, lax.rem(col, 2)

        def peer(offset):
            dy, dx, flip = offset
            return lax.rem(row + dy, outer_devs), lax.rem(chip + dx, chips) * 2 + lax.rem(core + flip, 2)

        def x_copy(e):
            return pltpu.make_async_copy(x_hbm.at[:, e], x_buf.at[e], x_sem.at[e])

        def gate_copy(e, f):
            cols = pl.ds(f * FF_CHUNK, FF_CHUNK)
            return pltpu.make_async_copy(wg_hbm.at[e, :, cols], wg_buf.at[e, :, cols], g_sem.at[e, f])

        def up_copy(e, f):
            cols = pl.ds(f * FF_CHUNK, FF_CHUNK)
            return pltpu.make_async_copy(wu_hbm.at[e, :, cols], wu_buf.at[e, :, cols], u_sem.at[e, f])

        def down_copy(e, d):
            cols = pl.ds(d * D_CHUNK, D_CHUNK)
            return pltpu.make_async_copy(wd_hbm.at[e, :, cols], wd_buf.at[e, :, cols], d_sem.at[e, d])

        def remote(e, offset):
            py, px = peer(offset)
            return pltpu.make_async_remote_copy(
                src_ref=send_buf.at[e, py * inner_devs + px], dst_ref=recv_buf.at[e, me],
                send_sem=send_sem.at[e], recv_sem=recv_sem.at[e],
                device_id={"outer": py, "expert": px}, device_id_type=MESH_ID)

        for e in range(experts):
            x_copy(e).start()
            for f in range(n_ff):
                gate_copy(e, f).start()
                up_copy(e, f).start()
            for d in range(n_d):
                down_copy(e, d).start()

        barrier = pltpu.get_barrier_semaphore()
        for offset in offsets:
            py, px = peer(offset)
            pl.semaphore_signal(barrier, inc=1, device_id={"outer": py, "expert": px}, device_id_type=MESH_ID)

        def expert_step(e):
            x_copy(e).wait()
            x_rows = x_buf[e].reshape(rows, width)
            for f in range(n_ff):
                cols = pl.ds(f * FF_CHUNK, FF_CHUNK)
                gate_copy(e, f).wait()
                gate_proj = jnp.dot(x_rows, wg_buf[e, :, cols], preferred_element_type=jnp.float32)
                up_copy(e, f).wait()
                up_proj = jnp.dot(x_rows, wu_buf[e, :, cols], preferred_element_type=jnp.float32)
                h_buf[:, cols] = (jax.nn.silu(gate_proj) * up_proj).astype(jnp.bfloat16)
            hidden = h_buf[...]
            for d in range(n_d):
                cols = pl.ds(d * D_CHUNK, D_CHUNK)
                down_copy(e, d).wait()
                y = jnp.dot(hidden, wd_buf[e, :, cols], preferred_element_type=jnp.float32)
                send_buf[e, :, :, cols] = y.reshape(group, capacity, D_CHUNK).astype(jnp.bfloat16)

        def send_step(e):
            for offset in offsets:
                remote(e, offset).start()
            recv_buf[e, me] = send_buf[e, me]

        expert_step(0)
        pl.semaphore_wait(barrier, group - 1)
        send_step(0)

        @pl.loop(1, experts)
        def _(e):
            expert_step(e)
            send_step(e)

        slots = slot_ref[...]
        keys = jnp.where(slots >= 0, eid_ref[...] * capacity + slots, -1)
        gates = gate_ref[...]
        line = lax.broadcasted_iota(jnp.int32, (rows, tokens), 0)
        for e in range(experts):
            row_key = (line // capacity) * (experts * capacity) + e * capacity + lax.rem(line, capacity)
            weight = jnp.zeros((rows, tokens), jnp.float32)
            for j in range(top):
                weight = weight + jnp.where(row_key == keys[j:j + 1], gates[j:j + 1], 0.0)
            used_buf[e] = jnp.broadcast_to(jnp.max(weight, axis=1, keepdims=True), (rows, 128))
            weight = weight.T
            high = jnp.minimum(weight, BF16_MAX).astype(jnp.bfloat16)
            rest = weight - high.astype(jnp.float32)
            mid = rest.astype(jnp.bfloat16)
            low = (rest - mid.astype(jnp.float32)).astype(jnp.bfloat16)
            w_buf[e, 0:tokens] = high
            w_buf[e, tokens:2 * tokens] = mid
            w_buf[e, 2 * tokens:3 * tokens] = low

        for e in range(experts):
            pltpu.make_async_remote_copy(
                src_ref=send_buf.at[e, pl.ds(0, group - 1)], dst_ref=recv_buf.at[e, pl.ds(0, group - 1)],
                send_sem=send_sem.at[e], recv_sem=recv_sem.at[e],
                device_id={"outer": row, "expert": col}, device_id_type=MESH_ID).wait_recv()
            used = used_buf[e] > 0.0
            for d in range(n_d):
                cols = pl.ds(d * D_CHUNK, D_CHUNK)
                y = recv_buf[e, :, :, cols].astype(jnp.float32).reshape(rows, D_CHUNK)
                y = jnp.where(jnp.concatenate([used] * (D_CHUNK // 128), axis=1), y, 0.0).astype(jnp.bfloat16)
                part = jnp.dot(w_buf[e], y, preferred_element_type=jnp.float32)
                total = part[0:tokens] + (part[tokens:2 * tokens] + part[2 * tokens:3 * tokens])
                if e > 0:
                    total = acc[:, cols] + total
                if e < experts - 1:
                    acc[:, cols] = total
                else:
                    out_ref[:, cols] = total.astype(jnp.bfloat16)

        for e in range(experts):
            pltpu.make_async_remote_copy(
                src_ref=send_buf.at[e, pl.ds(0, group - 1)], dst_ref=recv_buf.at[e, pl.ds(0, group - 1)],
                send_sem=send_sem.at[e], recv_sem=recv_sem.at[e],
                device_id={"outer": row, "expert": col}, device_id_type=MESH_ID).wait_send()

    return kernel


def solution(mesh):
    outer_devs = mesh.shape["outer"]
    inner_devs = mesh.shape["expert"]

    def local_step(x_disp, w_gate, w_up, w_down, slot_idx, expert_ids, gate_wts):
        group, experts, capacity, width = x_disp.shape
        ff = w_gate.shape[2]
        tokens, top = slot_idx.shape
        rows = group * capacity
        n_ff, n_d = ff // FF_CHUNK, width // D_CHUNK
        bf16, f32 = jnp.bfloat16, jnp.float32
        hbm = pl.BlockSpec(memory_space=pl.ANY)
        vmem = pl.BlockSpec(memory_space=pltpu.VMEM)
        return pl.pallas_call(
            make_kernel(outer_devs, inner_devs, experts, capacity, width, ff, tokens, top),
            out_shape=jax.ShapeDtypeStruct((tokens, width), bf16),
            in_specs=[hbm] * 4 + [vmem] * 3,
            out_specs=vmem,
            scratch_shapes=[
                pltpu.VMEM((experts, group, capacity, width), bf16),
                pltpu.VMEM((experts, width, ff), bf16),
                pltpu.VMEM((experts, width, ff), bf16),
                pltpu.VMEM((experts, ff, width), bf16),
                pltpu.VMEM((rows, ff), bf16),
                pltpu.VMEM((experts, group, capacity, width), bf16),
                pltpu.VMEM((experts, group, capacity, width), bf16),
                pltpu.VMEM((tokens, width), f32),
                pltpu.VMEM((experts, 3 * tokens, rows), bf16),
                pltpu.VMEM((experts, rows, 128), f32),
                pltpu.SemaphoreType.DMA((experts,)),
                pltpu.SemaphoreType.DMA((experts, n_ff)),
                pltpu.SemaphoreType.DMA((experts, n_ff)),
                pltpu.SemaphoreType.DMA((experts, n_d)),
                pltpu.SemaphoreType.DMA((experts,)),
                pltpu.SemaphoreType.DMA((experts,)),
            ],
            compiler_params=pltpu.CompilerParams(collective_id=0, has_side_effects=True, vmem_limit_bytes=67043328),
        )(x_disp, w_gate, w_up, w_down, slot_idx.T, expert_ids.T, gate_wts.T)

    expert_spec = P(("outer", "expert"))
    token_spec = P(("data", "outer", "expert"))
    return jax.shard_map(local_step, mesh=mesh, in_specs=(P("data", ("outer", "expert")), expert_spec, expert_spec, expert_spec, token_spec, token_spec, token_spec), out_specs=token_spec, check_vma=False)
```

```python
import jax
import jax.numpy as jnp
from jax import lax
from jax.experimental import pallas as pl
from jax.experimental.pallas import tpu as pltpu
from jax.sharding import PartitionSpec as P

MESH_ID = pl.DeviceIdType.MESH
CORES = 2
HALVES = 2
QUARTERS = 2
K_PARTS = 2
WEIGHT_SLOTS = 3
VMEM_LIMIT = 67043328
BF16_MAX = 3.3895313892515355e38


def make_kernel(ring, experts, capacity, width, ff, tokens, top):
    peers = ring * CORES
    group = ring * peers
    rows = group * capacity
    part_rows = experts * peers * capacity
    half = width // HALVES
    quarter = half // QUARTERS
    k_size = width // K_PARTS
    mid = tokens // 2

    def kernel(x_hbm, wg_hbm, wu_hbm, wd_hbm, slot_hbm, eid_hbm, gate_hbm, out_ref,
               x_buf, wg_buf, wu_buf, wd_buf, slot_buf, eid_buf, gate_buf, send_buf, recv_buf,
               routes, w_buf, used_buf, far_out, far_in, near_out, near_in, acc,
               x_sem, g_sem, u_sem, d_sem, route_sem, p1_send, p1_recv, rt_send, rt_recv,
               far_send, far_recv, own_send, own_recv, sum_send, sum_recv):
        row = lax.axis_index("outer")
        col = lax.axis_index("expert")
        chip, core = col // CORES, lax.rem(col, CORES)
        place = (row, chip)
        source = (col, row * CORES + core)

        def shift(start, step):
            return lax.rem(start + step, ring)

        def ring_peer(h, step):
            if h == 0:
                return {"outer": shift(row, step), "expert": col}
            return {"outer": row, "expert": shift(chip, step) * CORES + core}

        def first_peer(h, step, flip):
            other = lax.rem(core + flip, CORES)
            if h == 0:
                to = shift(chip, step)
                return {"outer": row, "expert": to * CORES + other}, to, other
            to = shift(row, step)
            return {"outer": to, "expert": chip * CORES + other}, to, other

        def rows_for(h, e, to, other, cols):
            if h == 0:
                return send_buf.at[e, :, to, other, :, cols]
            return send_buf.at[e, to, :, other, :, cols]

        hops = [(2, 0), (2, 1), (1, 0), (ring - 1, 0), (1, 1), (ring - 1, 1), (0, 1)]

        def first_copy(h, e, q, step, flip):
            peer, to, other = first_peer(h, step, flip)
            return pltpu.make_async_remote_copy(
                src_ref=rows_for(h, e, to, other, pl.ds(h * half + q * quarter, quarter)),
                dst_ref=recv_buf.at[h, e, source[h], :, :, pl.ds(q * quarter, quarter)],
                send_sem=p1_send.at[h, e, q], recv_sem=p1_recv.at[h, e, q],
                device_id=peer, device_id_type=MESH_ID)

        def first_all(h, e, q):
            ref = recv_buf.at[h, e, pl.ds(0, peers - 1), :, :, pl.ds(q * quarter, quarter)]
            return pltpu.make_async_remote_copy(
                src_ref=ref, dst_ref=ref, send_sem=p1_send.at[h, e, q], recv_sem=p1_recv.at[h, e, q],
                device_id=ring_peer(h, 1), device_id_type=MESH_ID)

        def route_copy(h, step):
            return pltpu.make_async_remote_copy(
                src_ref=routes.at[h, 0], dst_ref=routes.at[h, ring - step],
                send_sem=rt_send.at[0], recv_sem=rt_recv.at[0],
                device_id=ring_peer(h, step), device_id_type=MESH_ID)

        def route_all():
            ref = routes.at[:, pl.ds(1, ring - 1)]
            return pltpu.make_async_remote_copy(
                src_ref=ref, dst_ref=ref, send_sem=rt_send.at[0], recv_sem=rt_recv.at[0],
                device_id=ring_peer(0, 1), device_id_type=MESH_ID)

        def near_step(way):
            return 1 if way == 0 else ring - 1

        def relay_part(way):
            return pl.ds(way * mid, mid)

        def own_part(way):
            return pl.ds((1 - way) * mid, mid)

        def far_copy(h, q, way):
            return pltpu.make_async_remote_copy(
                src_ref=far_out.at[h, q, way], dst_ref=far_in.at[h, q, way],
                send_sem=far_send.at[h, q, way], recv_sem=far_recv.at[h, q, way],
                device_id=ring_peer(h, near_step(way)), device_id_type=MESH_ID)

        def own_copy(h, q, way):
            return pltpu.make_async_remote_copy(
                src_ref=near_out.at[h, q, way, own_part(way)], dst_ref=near_in.at[h, q, way, own_part(way)],
                send_sem=own_send.at[h, q, way], recv_sem=own_recv.at[h, q, way],
                device_id=ring_peer(h, near_step(way)), device_id_type=MESH_ID)

        def sum_copy(h, q, way):
            return pltpu.make_async_remote_copy(
                src_ref=near_out.at[h, q, way, relay_part(way)], dst_ref=near_in.at[h, q, way, relay_part(way)],
                send_sem=sum_send.at[h, q, way], recv_sem=sum_recv.at[h, q, way],
                device_id=ring_peer(h, near_step(way)), device_id_type=MESH_ID)

        def part_copies(k):
            cols = pl.ds(k * k_size, k_size)
            return (pltpu.make_async_copy(x_hbm.at[:, 0, :, cols], x_buf.at[0, :, :, cols], x_sem.at[k]),
                    pltpu.make_async_copy(wg_hbm.at[0, cols], wg_buf.at[0, cols], g_sem.at[k]),
                    pltpu.make_async_copy(wu_hbm.at[0, cols], wu_buf.at[0, cols], u_sem.at[k]))

        def down_part_copy(h):
            cols = pl.ds(h * half, half)
            return pltpu.make_async_copy(wd_hbm.at[0, :, cols], wd_buf.at[0, :, cols], d_sem.at[h])

        def weight_copies(e):
            slot = lax.rem(e, WEIGHT_SLOTS)
            return (pltpu.make_async_copy(x_hbm.at[:, e], x_buf.at[slot], x_sem.at[K_PARTS + e]),
                    pltpu.make_async_copy(wg_hbm.at[e], wg_buf.at[slot], g_sem.at[K_PARTS + e]),
                    pltpu.make_async_copy(wu_hbm.at[e], wu_buf.at[slot], u_sem.at[K_PARTS + e]),
                    pltpu.make_async_copy(wd_hbm.at[e], wd_buf.at[slot], d_sem.at[HALVES + e]))

        def token_copies():
            return (pltpu.make_async_copy(slot_hbm, slot_buf, route_sem.at[0]),
                    pltpu.make_async_copy(eid_hbm, eid_buf, route_sem.at[1]),
                    pltpu.make_async_copy(gate_hbm, gate_buf, route_sem.at[2]))

        for k in range(K_PARTS):
            for copy in part_copies(k):
                copy.start()
        greet = [first_peer(h, step, flip)[0] for h in range(HALVES) for step, flip in hops[:-1]] + [first_peer(0, 0, 1)[0]]
        barrier = pltpu.get_barrier_semaphore()
        for peer in greet:
            pl.semaphore_signal(barrier, inc=1, device_id=peer, device_id_type=MESH_ID)
        for h in range(HALVES):
            down_part_copy(h).start()
        for copy in token_copies():
            copy.start()
        for e in range(1, WEIGHT_SLOTS):
            for copy in weight_copies(e):
                copy.start()

        def first_send(h, e):
            for q in range(QUARTERS):
                for step, flip in hops:
                    first_copy(h, e, q, step, flip).start()
            cols = pl.ds(h * half, half)
            if h == 0:
                recv_buf[h, e, source[h]] = send_buf[e, :, chip, core, :, cols]
            else:
                recv_buf[h, e, source[h]] = send_buf[e, row, :, core, :, cols]

        def activation(gate_proj, up_proj):
            return (jax.nn.silu(gate_proj) * up_proj).astype(jnp.bfloat16)

        def down_step(e, slot, h, hidden):
            cols = pl.ds(h * half, half)
            y = jnp.dot(hidden, wd_buf[slot, :, cols], preferred_element_type=jnp.float32)
            send_buf[e, :, :, :, :, cols] = y.reshape(ring, ring, CORES, capacity, half).astype(jnp.bfloat16)

        gate_proj = up_proj = None
        for k in range(K_PARTS):
            for copy in part_copies(k):
                copy.wait()
            cols = pl.ds(k * k_size, k_size)
            x_rows = x_buf[0, :, :, cols].reshape(rows, k_size)
            gate_part = jnp.dot(x_rows, wg_buf[0, cols], preferred_element_type=jnp.float32)
            up_part = jnp.dot(x_rows, wu_buf[0, cols], preferred_element_type=jnp.float32)
            gate_proj = gate_part if gate_proj is None else gate_proj + gate_part
            up_proj = up_part if up_proj is None else up_proj + up_part
        hidden = activation(gate_proj, up_proj)
        for h in range(HALVES):
            down_part_copy(h).wait()
            down_step(0, 0, h, hidden)
            if h == 0:
                pl.semaphore_wait(barrier, len(greet))
            first_send(h, 0)
        for e in range(WEIGHT_SLOTS, experts):
            for copy in weight_copies(e):
                copy.start()

        for copy in token_copies():
            copy.wait()
        slots = slot_buf[...]
        keys = jnp.where(slots >= 0, eid_buf[...] * capacity + slots, -1).astype(jnp.float32)
        for h in range(HALVES):
            routes[h, 0, 0:top] = keys
            routes[h, 0, top:2 * top] = gate_buf[...]
        for h in range(HALVES):
            for step in range(1, ring):
                route_copy(h, step).start()

        @pl.loop(1, experts)
        def _(e):
            slot = lax.rem(e, WEIGHT_SLOTS)
            x_copy, gate_copy, up_copy, down_copy = weight_copies(e)
            x_copy.wait()
            x_rows = x_buf[slot].reshape(rows, width)
            gate_copy.wait()
            gate_proj = jnp.dot(x_rows, wg_buf[slot], preferred_element_type=jnp.float32)
            up_copy.wait()
            up_proj = jnp.dot(x_rows, wu_buf[slot], preferred_element_type=jnp.float32)
            hidden = activation(gate_proj, up_proj)
            down_copy.wait()
            for h in range(HALVES):
                down_step(e, slot, h, hidden)
                first_send(h, e)

        route_all().wait_recv()
        line = lax.broadcasted_iota(jnp.int32, (part_rows, tokens), 0)
        local = line // (peers * capacity)
        src = lax.rem(line // capacity, peers)
        device = (row * peers + src, (src // CORES) * peers + chip * CORES + lax.rem(src, CORES))
        for h in range(HALVES):
            row_key = ((device[h] * experts + local) * capacity + lax.rem(line, capacity)).astype(jnp.float32)
            for step in range(ring):
                weight = jnp.zeros((part_rows, tokens), jnp.float32)
                for j in range(top):
                    weight = weight + jnp.where(row_key == routes[h, step, j:j + 1], routes[h, step, top + j:top + j + 1], 0.0)
                used_buf[h, step] = jnp.broadcast_to(jnp.max(weight, axis=1, keepdims=True), (part_rows, 128))
                weight = weight.T
                high = jnp.minimum(weight, BF16_MAX).astype(jnp.bfloat16)
                rest = weight - high.astype(jnp.float32)
                middle = rest.astype(jnp.bfloat16)
                low = (rest - middle.astype(jnp.float32)).astype(jnp.bfloat16)
                w_buf[h, step, 0:tokens] = high
                w_buf[h, step, tokens:2 * tokens] = middle
                w_buf[h, step, 2 * tokens:3 * tokens] = low

        def partial(h, q, step):
            y = recv_buf[h, :, :, shift(place[h], step), :, pl.ds(q * quarter, quarter)]
            y = y.astype(jnp.float32).reshape(part_rows, quarter)
            used = used_buf[h, step] > 0.0
            y = jnp.where(jnp.concatenate([used] * (quarter // 128), axis=1), y, 0.0).astype(jnp.bfloat16)
            part = jnp.dot(w_buf[h, step], y, preferred_element_type=jnp.float32)
            return part[0:tokens] + (part[tokens:2 * tokens] + part[2 * tokens:3 * tokens])

        blocks = [(h, q) for q in range(QUARTERS) for h in range(HALVES)]
        for h, q in blocks:
            for e in range(experts):
                first_all(h, e, q).wait_recv()
            far = partial(h, q, 2)
            for way in range(2):
                far_out[h, q, way] = far[way * mid:(way + 1) * mid]
                far_copy(h, q, way).start()
            for way in range(2):
                near_out[h, q, way] = partial(h, q, near_step(way))
                own_copy(h, q, way).start()
        for h, q in blocks:
            for way in range(2):
                far_copy(h, q, way).wait_recv()
                near_out[h, q, way, relay_part(way)] = near_out[h, q, way, relay_part(way)] + far_in[h, q, way]
                sum_copy(h, q, way).start()
            acc[:, pl.ds(h * half + q * quarter, quarter)] = partial(h, q, 0)
        for h, q in blocks:
            for way in range(2):
                own_copy(h, q, way).wait_recv()
                sum_copy(h, q, way).wait_recv()
            cols = pl.ds(h * half + q * quarter, quarter)
            out_ref[:, cols] = (acc[:, cols] + near_in[h, q, 0] + near_in[h, q, 1]).astype(jnp.bfloat16)

        route_all().wait_send()
        for h, q in blocks:
            for e in range(experts):
                first_all(h, e, q).wait_send()
            for way in range(2):
                far_copy(h, q, way).wait_send()
                own_copy(h, q, way).wait_send()
                sum_copy(h, q, way).wait_send()

    return kernel


def solution(mesh):
    outer_devs = mesh.shape["outer"]
    inner_devs = mesh.shape["expert"]
    assert inner_devs == outer_devs * CORES and outer_devs == 4

    def local_step(x_disp, w_gate, w_up, w_down, slot_idx, expert_ids, gate_wts):
        group, experts, capacity, width = x_disp.shape
        ff = w_gate.shape[2]
        tokens, top = slot_idx.shape
        rows = group * capacity
        ring = outer_devs
        peers = inner_devs
        half = width // HALVES
        quarter = half // QUARTERS
        bf16, f32 = jnp.bfloat16, jnp.float32
        hbm = pl.BlockSpec(memory_space=pltpu.HBM)
        dma = pltpu.SemaphoreType.DMA
        return pl.pallas_call(
            make_kernel(ring, experts, capacity, width, ff, tokens, top),
            out_shape=jax.ShapeDtypeStruct((tokens, width), bf16),
            in_specs=[hbm] * 7,
            out_specs=pl.BlockSpec(memory_space=pltpu.VMEM),
            scratch_shapes=[
                pltpu.VMEM((WEIGHT_SLOTS, group, capacity, width), bf16),
                pltpu.VMEM((WEIGHT_SLOTS, width, ff), bf16),
                pltpu.VMEM((WEIGHT_SLOTS, width, ff), bf16),
                pltpu.VMEM((WEIGHT_SLOTS, ff, width), bf16),
                pltpu.VMEM((top, tokens), jnp.int32),
                pltpu.VMEM((top, tokens), jnp.int32),
                pltpu.VMEM((top, tokens), f32),
                pltpu.VMEM((experts, ring, ring, CORES, capacity, width), bf16),
                pltpu.VMEM((HALVES, experts, peers, ring, capacity, half), bf16),
                pltpu.VMEM((HALVES, ring, 2 * top, tokens), f32),
                pltpu.VMEM((HALVES, ring, 3 * tokens, experts * peers * capacity), bf16),
                pltpu.VMEM((HALVES, ring, experts * peers * capacity, 128), f32),
                pltpu.VMEM((HALVES, QUARTERS, 2, tokens // 2, quarter), f32),
                pltpu.VMEM((HALVES, QUARTERS, 2, tokens // 2, quarter), f32),
                pltpu.VMEM((HALVES, QUARTERS, 2, tokens, quarter), f32),
                pltpu.VMEM((HALVES, QUARTERS, 2, tokens, quarter), f32),
                pltpu.VMEM((tokens, width), f32),
                dma((K_PARTS + experts,)),
                dma((K_PARTS + experts,)),
                dma((K_PARTS + experts,)),
                dma((HALVES + experts,)),
                dma((3,)),
                dma((HALVES, experts, QUARTERS)),
                dma((HALVES, experts, QUARTERS)),
                dma((1,)),
                dma((1,)),
                dma((HALVES, QUARTERS, 2)),
                dma((HALVES, QUARTERS, 2)),
                dma((HALVES, QUARTERS, 2)),
                dma((HALVES, QUARTERS, 2)),
                dma((HALVES, QUARTERS, 2)),
                dma((HALVES, QUARTERS, 2)),
            ],
            compiler_params=pltpu.CompilerParams(collective_id=0, has_side_effects=True, vmem_limit_bytes=VMEM_LIMIT),
        )(x_disp, w_gate, w_up, w_down, slot_idx.T, expert_ids.T, gate_wts.T)

    expert_spec = P(("outer", "expert"))
    token_spec = P(("data", "outer", "expert"))
    return jax.shard_map(local_step, mesh=mesh, in_specs=(P("data", ("outer", "expert")), expert_spec, expert_spec, expert_spec, token_spec, token_spec, token_spec), out_specs=token_spec, check_vma=False)
```

```python
import jax
import jax.numpy as jnp
from jax import lax
from jax.experimental import pallas as pl
from jax.experimental.pallas import tpu as pltpu
from jax.sharding import PartitionSpec as P

MESH_ID = pl.DeviceIdType.MESH
CORES = 2
HALVES = 2
QUARTERS = 2
K_PARTS = 4
WEIGHT_SLOTS = 3
VMEM_LIMIT = 62 * 2 ** 20
BF16_MAX = 3.3895313892515355e38


def make_kernel(ring, experts, capacity, width, ff, tokens, top):
    peers = ring * CORES
    group = ring * peers
    rows = group * capacity
    part_rows = experts * peers * capacity
    half = width // HALVES
    quarter = half // QUARTERS
    k_size = width // K_PARTS
    mid = tokens // 2

    def kernel(x_hbm, wg_hbm, wu_hbm, wd_hbm, slot_hbm, eid_hbm, gate_hbm, out_ref,
               x_buf, wg_buf, wu_buf, wd_buf, slot_buf, eid_buf, gate_buf, send_buf, recv_buf,
               routes, w_buf, used_buf, far_out, far_in, near_out, near_in, acc,
               x_sem, g_sem, u_sem, d_sem, route_sem, p1_send, p1_recv, rt_send, rt_recv,
               far_send, far_recv, own_send, own_recv, sum_send, sum_recv):
        row = lax.axis_index("outer")
        col = lax.axis_index("expert")
        chip, core = col // CORES, lax.rem(col, CORES)
        blocks = [(h, q) for q in range(QUARTERS) for h in range(HALVES)]
        place = (row, chip)
        source = (col, row * CORES + core)

        def shift(start, step):
            return lax.rem(start + step, ring)

        def ring_peer(h, step):
            if h == 0:
                return {"outer": shift(row, step), "expert": col}
            return {"outer": row, "expert": shift(chip, step) * CORES + core}

        def first_peer(h, step, flip):
            other = lax.rem(core + flip, CORES)
            if h == 0:
                to = shift(chip, step)
                return {"outer": row, "expert": to * CORES + other}, to, other
            to = shift(row, step)
            return {"outer": to, "expert": chip * CORES + other}, to, other

        def rows_for(h, e, to, other, cols):
            if h == 0:
                return send_buf.at[e, :, to, other, :, cols]
            return send_buf.at[e, to, :, other, :, cols]

        hops = [(2, 0), (2, 1), (1, 0), (ring - 1, 0), (1, 1), (ring - 1, 1), (0, 1)]

        def first_copy(h, e, q, step, flip):
            peer, to, other = first_peer(h, step, flip)
            return pltpu.make_async_remote_copy(
                src_ref=rows_for(h, e, to, other, pl.ds(h * half + q * quarter, quarter)),
                dst_ref=recv_buf.at[h, e, source[h], :, :, pl.ds(q * quarter, quarter)],
                send_sem=p1_send.at[h, e, q], recv_sem=p1_recv.at[h, e, q],
                device_id=peer, device_id_type=MESH_ID)

        def first_all(h, e, q):
            ref = recv_buf.at[h, e, pl.ds(0, peers - 1), :, :, pl.ds(q * quarter, quarter)]
            return pltpu.make_async_remote_copy(
                src_ref=ref, dst_ref=ref, send_sem=p1_send.at[h, e, q], recv_sem=p1_recv.at[h, e, q],
                device_id=ring_peer(h, 1), device_id_type=MESH_ID)

        def route_copy(h, step):
            return pltpu.make_async_remote_copy(
                src_ref=routes.at[h, 0], dst_ref=routes.at[h, ring - step],
                send_sem=rt_send.at[0], recv_sem=rt_recv.at[0],
                device_id=ring_peer(h, step), device_id_type=MESH_ID)

        def route_all():
            ref = routes.at[:, pl.ds(1, ring - 1)]
            return pltpu.make_async_remote_copy(
                src_ref=ref, dst_ref=ref, send_sem=rt_send.at[0], recv_sem=rt_recv.at[0],
                device_id=ring_peer(0, 1), device_id_type=MESH_ID)

        def near_step(way):
            return 1 if way == 0 else ring - 1

        def relay_part(way):
            return pl.ds(way * mid, mid)

        def own_part(way):
            return pl.ds((1 - way) * mid, mid)

        def far_copy(h, q, way):
            return pltpu.make_async_remote_copy(
                src_ref=far_out.at[h, q, way], dst_ref=far_in.at[h, q, way],
                send_sem=far_send.at[h, q, way], recv_sem=far_recv.at[h, q, way],
                device_id=ring_peer(h, near_step(way)), device_id_type=MESH_ID)

        def own_copy(h, q, way):
            return pltpu.make_async_remote_copy(
                src_ref=near_out.at[h, q, way, own_part(way)], dst_ref=near_in.at[h, q, way, own_part(way)],
                send_sem=own_send.at[h, q, way], recv_sem=own_recv.at[h, q, way],
                device_id=ring_peer(h, near_step(way)), device_id_type=MESH_ID)

        def sum_copy(h, q, way):
            return pltpu.make_async_remote_copy(
                src_ref=near_out.at[h, q, way, relay_part(way)], dst_ref=near_in.at[h, q, way, relay_part(way)],
                send_sem=sum_send.at[h, q, way], recv_sem=sum_recv.at[h, q, way],
                device_id=ring_peer(h, near_step(way)), device_id_type=MESH_ID)

        def part_copies(k):
            cols = pl.ds(k * k_size, k_size)
            return (pltpu.make_async_copy(x_hbm.at[:, 0, :, cols], x_buf.at[0, :, :, cols], x_sem.at[k]),
                    pltpu.make_async_copy(wg_hbm.at[0, cols], wg_buf.at[0, cols], g_sem.at[k]),
                    pltpu.make_async_copy(wu_hbm.at[0, cols], wu_buf.at[0, cols], u_sem.at[k]))

        def down_part_copy(h, q):
            cols = pl.ds(h * half + q * quarter, quarter)
            return pltpu.make_async_copy(wd_hbm.at[0, :, cols], wd_buf.at[0, :, cols], d_sem.at[h * QUARTERS + q])

        def weight_copies(e):
            slot = lax.rem(e, WEIGHT_SLOTS)
            return (pltpu.make_async_copy(x_hbm.at[:, e], x_buf.at[slot], x_sem.at[K_PARTS + e]),
                    pltpu.make_async_copy(wg_hbm.at[e], wg_buf.at[slot], g_sem.at[K_PARTS + e]),
                    pltpu.make_async_copy(wu_hbm.at[e], wu_buf.at[slot], u_sem.at[K_PARTS + e]),
                    pltpu.make_async_copy(wd_hbm.at[e], wd_buf.at[slot], d_sem.at[HALVES * QUARTERS + e]))

        def token_copies():
            return (pltpu.make_async_copy(slot_hbm, slot_buf, route_sem.at[0]),
                    pltpu.make_async_copy(eid_hbm, eid_buf, route_sem.at[1]),
                    pltpu.make_async_copy(gate_hbm, gate_buf, route_sem.at[2]))

        for k in range(K_PARTS):
            for copy in part_copies(k):
                copy.start()
        greet = [first_peer(h, step, flip)[0] for h in range(HALVES) for step, flip in hops[:-1]] + [first_peer(0, 0, 1)[0]]
        barrier = pltpu.get_barrier_semaphore()
        for peer in greet:
            pl.semaphore_signal(barrier, inc=1, device_id=peer, device_id_type=MESH_ID)
        for h, q in blocks:
            down_part_copy(h, q).start()
        for copy in token_copies():
            copy.start()
        for e in range(1, WEIGHT_SLOTS):
            for copy in weight_copies(e):
                copy.start()

        def first_send(h, q, e):
            for step, flip in hops:
                first_copy(h, e, q, step, flip).start()

        def keep_own(h, e):
            cols = pl.ds(h * half, half)
            if h == 0:
                recv_buf[h, e, source[h]] = send_buf[e, :, chip, core, :, cols]
            else:
                recv_buf[h, e, source[h]] = send_buf[e, row, :, core, :, cols]

        def activation(gate_proj, up_proj):
            return (jax.nn.silu(gate_proj) * up_proj).astype(jnp.bfloat16)

        def down_step(e, slot, start, size, hidden):
            cols = pl.ds(start, size)
            y = jnp.dot(hidden, wd_buf[slot, :, cols], preferred_element_type=jnp.float32)
            send_buf[e, :, :, :, :, cols] = y.reshape(ring, ring, CORES, capacity, size).astype(jnp.bfloat16)

        gate_proj = up_proj = None
        for k in range(K_PARTS):
            for copy in part_copies(k):
                copy.wait()
            cols = pl.ds(k * k_size, k_size)
            x_rows = x_buf[0, :, :, cols].reshape(rows, k_size)
            gate_part = jnp.dot(x_rows, wg_buf[0, cols], preferred_element_type=jnp.float32)
            up_part = jnp.dot(x_rows, wu_buf[0, cols], preferred_element_type=jnp.float32)
            gate_proj = gate_part if gate_proj is None else gate_proj + gate_part
            up_proj = up_part if up_proj is None else up_proj + up_part
        hidden = activation(gate_proj, up_proj)
        for h, q in blocks:
            down_part_copy(h, q).wait()
            down_step(0, 0, h * half + q * quarter, quarter, hidden)
            if (h, q) == blocks[0]:
                pl.semaphore_wait(barrier, len(greet))
            first_send(h, q, 0)
        for h in range(HALVES):
            keep_own(h, 0)
        for e in range(WEIGHT_SLOTS, experts):
            for copy in weight_copies(e):
                copy.start()

        for copy in token_copies():
            copy.wait()
        slots = slot_buf[...]
        keys = jnp.where(slots >= 0, eid_buf[...] * capacity + slots, -1).astype(jnp.float32)
        for h in range(HALVES):
            routes[h, 0, 0:top] = keys
            routes[h, 0, top:2 * top] = gate_buf[...]
        for h in range(HALVES):
            for step in range(1, ring):
                route_copy(h, step).start()

        @pl.loop(1, experts)
        def _(e):
            slot = lax.rem(e, WEIGHT_SLOTS)
            x_copy, gate_copy, up_copy, down_copy = weight_copies(e)
            x_copy.wait()
            x_rows = x_buf[slot].reshape(rows, width)
            gate_copy.wait()
            gate_proj = jnp.dot(x_rows, wg_buf[slot], preferred_element_type=jnp.float32)
            up_copy.wait()
            up_proj = jnp.dot(x_rows, wu_buf[slot], preferred_element_type=jnp.float32)
            hidden = activation(gate_proj, up_proj)
            down_copy.wait()
            for h in range(HALVES):
                down_step(e, slot, h * half, half, hidden)
                for q in range(QUARTERS):
                    first_send(h, q, e)
            for h in range(HALVES):
                keep_own(h, e)

        route_all().wait_recv()
        line = lax.broadcasted_iota(jnp.int32, (part_rows, tokens), 0)
        local = line // (peers * capacity)
        src = lax.rem(line // capacity, peers)
        device = (row * peers + src, (src // CORES) * peers + chip * CORES + lax.rem(src, CORES))
        for h in range(HALVES):
            row_key = ((device[h] * experts + local) * capacity + lax.rem(line, capacity)).astype(jnp.float32)
            for step in range(ring):
                weight = jnp.zeros((part_rows, tokens), jnp.float32)
                for j in range(top):
                    weight = weight + jnp.where(row_key == routes[h, step, j:j + 1], routes[h, step, top + j:top + j + 1], 0.0)
                used_buf[h, step] = jnp.broadcast_to(jnp.max(weight, axis=1, keepdims=True), (part_rows, 128))
                weight = weight.T
                high = jnp.minimum(weight, BF16_MAX).astype(jnp.bfloat16)
                rest = weight - high.astype(jnp.float32)
                middle = rest.astype(jnp.bfloat16)
                low = (rest - middle.astype(jnp.float32)).astype(jnp.bfloat16)
                w_buf[h, step, 0:tokens] = high
                w_buf[h, step, tokens:2 * tokens] = middle
                w_buf[h, step, 2 * tokens:3 * tokens] = low

        def partial(h, q, step):
            y = recv_buf[h, :, :, shift(place[h], step), :, pl.ds(q * quarter, quarter)]
            y = y.astype(jnp.float32).reshape(part_rows, quarter)
            used = used_buf[h, step] > 0.0
            y = jnp.where(jnp.concatenate([used] * (quarter // 128), axis=1), y, 0.0).astype(jnp.bfloat16)
            part = jnp.dot(w_buf[h, step], y, preferred_element_type=jnp.float32)
            return part[0:tokens] + (part[tokens:2 * tokens] + part[2 * tokens:3 * tokens])

        for h, q in blocks:
            for e in range(experts):
                first_all(h, e, q).wait_recv()
            far = partial(h, q, 2)
            for way in range(2):
                far_out[h, q, way] = far[way * mid:(way + 1) * mid]
                far_copy(h, q, way).start()
            for way in range(2):
                near_out[h, q, way] = partial(h, q, near_step(way))
                own_copy(h, q, way).start()
        for h, q in blocks:
            for way in range(2):
                far_copy(h, q, way).wait_recv()
                near_out[h, q, way, relay_part(way)] = near_out[h, q, way, relay_part(way)] + far_in[h, q, way]
                sum_copy(h, q, way).start()
            acc[:, pl.ds(h * half + q * quarter, quarter)] = partial(h, q, 0)
        for h, q in blocks:
            for way in range(2):
                own_copy(h, q, way).wait_recv()
                sum_copy(h, q, way).wait_recv()
            cols = pl.ds(h * half + q * quarter, quarter)
            out_ref[:, cols] = (acc[:, cols] + near_in[h, q, 0] + near_in[h, q, 1]).astype(jnp.bfloat16)

        route_all().wait_send()
        for h, q in blocks:
            for e in range(experts):
                first_all(h, e, q).wait_send()
            for way in range(2):
                far_copy(h, q, way).wait_send()
                own_copy(h, q, way).wait_send()
                sum_copy(h, q, way).wait_send()

    return kernel


def solution(mesh):
    outer_devs = mesh.shape["outer"]
    inner_devs = mesh.shape["expert"]
    assert inner_devs == outer_devs * CORES and outer_devs == 4

    def local_step(x_disp, w_gate, w_up, w_down, slot_idx, expert_ids, gate_wts):
        group, experts, capacity, width = x_disp.shape
        ff = w_gate.shape[2]
        tokens, top = slot_idx.shape
        rows = group * capacity
        ring = outer_devs
        peers = inner_devs
        half = width // HALVES
        quarter = half // QUARTERS
        bf16, f32 = jnp.bfloat16, jnp.float32
        hbm = pl.BlockSpec(memory_space=pltpu.HBM)
        dma = pltpu.SemaphoreType.DMA
        return pl.pallas_call(
            make_kernel(ring, experts, capacity, width, ff, tokens, top),
            out_shape=pltpu.VMEM((tokens, width), bf16),
            in_specs=[hbm] * 7,
            out_specs=pl.BlockSpec(memory_space=pltpu.VMEM),
            scratch_shapes=[
                pltpu.VMEM((WEIGHT_SLOTS, group, capacity, width), bf16),
                pltpu.VMEM((WEIGHT_SLOTS, width, ff), bf16),
                pltpu.VMEM((WEIGHT_SLOTS, width, ff), bf16),
                pltpu.VMEM((WEIGHT_SLOTS, ff, width), bf16),
                pltpu.VMEM((top, tokens), jnp.int32),
                pltpu.VMEM((top, tokens), jnp.int32),
                pltpu.VMEM((top, tokens), f32),
                pltpu.VMEM((experts, ring, ring, CORES, capacity, width), bf16),
                pltpu.VMEM((HALVES, experts, peers, ring, capacity, half), bf16),
                pltpu.VMEM((HALVES, ring, 2 * top, tokens), f32),
                pltpu.VMEM((HALVES, ring, 3 * tokens, experts * peers * capacity), bf16),
                pltpu.VMEM((HALVES, ring, experts * peers * capacity, 128), f32),
                pltpu.VMEM((HALVES, QUARTERS, 2, tokens // 2, quarter), f32),
                pltpu.VMEM((HALVES, QUARTERS, 2, tokens // 2, quarter), f32),
                pltpu.VMEM((HALVES, QUARTERS, 2, tokens, quarter), f32),
                pltpu.VMEM((HALVES, QUARTERS, 2, tokens, quarter), f32),
                pltpu.VMEM((tokens, width), f32),
                dma((K_PARTS + experts,)),
                dma((K_PARTS + experts,)),
                dma((K_PARTS + experts,)),
                dma((HALVES * QUARTERS + experts,)),
                dma((3,)),
                dma((HALVES, experts, QUARTERS)),
                dma((HALVES, experts, QUARTERS)),
                dma((1,)),
                dma((1,)),
                dma((HALVES, QUARTERS, 2)),
                dma((HALVES, QUARTERS, 2)),
                dma((HALVES, QUARTERS, 2)),
                dma((HALVES, QUARTERS, 2)),
                dma((HALVES, QUARTERS, 2)),
                dma((HALVES, QUARTERS, 2)),
            ],
            compiler_params=pltpu.CompilerParams(collective_id=0, has_side_effects=True, vmem_limit_bytes=VMEM_LIMIT),
        )(x_disp, w_gate, w_up, w_down, slot_idx.T, expert_ids.T, gate_wts.T)

    expert_spec = P(("outer", "expert"))
    token_spec = P(("data", "outer", "expert"))
    return jax.shard_map(local_step, mesh=mesh, in_specs=(P("data", ("outer", "expert")), expert_spec, expert_spec, expert_spec, token_spec, token_spec, token_spec), out_specs=token_spec, check_vma=False)
```

```python
import jax
import jax.numpy as jnp
from jax import lax
from jax.experimental import pallas as pl
from jax.experimental.pallas import tpu as pltpu
from jax.sharding import PartitionSpec as P

MESH_ID = pl.DeviceIdType.MESH
CORES = 2
HALVES = 2
QUARTERS = 2
K_PARTS = 4
WEIGHT_SLOTS = 3
VMEM_LIMIT = 62 * 2 ** 20
BF16_MAX = 3.3895313892515355e38


def make_kernel(ring, experts, capacity, width, ff, tokens, top):
    peers = ring * CORES
    group = ring * peers
    rows = group * capacity
    part_rows = experts * peers * capacity
    half = width // HALVES
    quarter = half // QUARTERS
    k_size = width // K_PARTS
    mid = tokens // 2

    def kernel(x_hbm, wg_hbm, wu_hbm, wd_hbm, slot_hbm, eid_hbm, gate_hbm, out_ref,
               x_buf, wg_buf, wu_buf, wd_buf, slot_buf, eid_buf, gate_buf, send_buf, recv_buf,
               routes, w_buf, used_buf, far_out, far_in, near_out, near_in, acc,
               part_sem, down_sem, weight_sem, token_sem, first_out, first_in, route_out, route_in,
               far_sent, far_here, near_sent, own_here, sum_here):
        row = lax.axis_index("outer")
        col = lax.axis_index("expert")
        chip, core = col // CORES, lax.rem(col, CORES)
        blocks = [(h, q) for q in range(QUARTERS) for h in range(HALVES)]
        place = (row, chip)
        source = (col, row * CORES + core)

        def shift(start, step):
            return lax.rem(start + step, ring)

        def ring_peer(h, step):
            if h == 0:
                return {"outer": shift(row, step), "expert": col}
            return {"outer": row, "expert": shift(chip, step) * CORES + core}

        def first_peer(h, step, flip):
            other = lax.rem(core + flip, CORES)
            if h == 0:
                to = shift(chip, step)
                return {"outer": row, "expert": to * CORES + other}, to, other
            to = shift(row, step)
            return {"outer": to, "expert": chip * CORES + other}, to, other

        def rows_for(h, e, to, other, cols):
            if h == 0:
                return send_buf.at[e, :, to, other, :, cols]
            return send_buf.at[e, to, :, other, :, cols]

        hops = [(2, 0), (2, 1), (1, 0), (ring - 1, 0), (1, 1), (ring - 1, 1), (0, 1)]

        def first_copy(h, e, q, step, flip):
            peer, to, other = first_peer(h, step, flip)
            return pltpu.make_async_remote_copy(
                src_ref=rows_for(h, e, to, other, pl.ds(h * half + q * quarter, quarter)),
                dst_ref=recv_buf.at[h, e, source[h], :, :, pl.ds(q * quarter, quarter)],
                send_sem=first_out.at[0], recv_sem=first_in.at[h, q],
                device_id=peer, device_id_type=MESH_ID)

        def whole(ref, sent, here):
            return pltpu.make_async_remote_copy(
                src_ref=ref, dst_ref=ref, send_sem=sent, recv_sem=here,
                device_id=ring_peer(0, 1), device_id_type=MESH_ID)

        def first_here(h, q):
            ref = recv_buf.at[h, :, pl.ds(0, peers - 1), :, :, pl.ds(q * quarter, quarter)]
            return whole(ref, first_out.at[0], first_in.at[h, q])

        def first_sent():
            return whole(recv_buf.at[:, :, pl.ds(0, peers - 1)], first_out.at[0], first_in.at[0, 0])

        def route_copy(h, step):
            return pltpu.make_async_remote_copy(
                src_ref=routes.at[h, 0], dst_ref=routes.at[h, ring - step],
                send_sem=route_out.at[0], recv_sem=route_in.at[0],
                device_id=ring_peer(h, step), device_id_type=MESH_ID)

        def route_all():
            ref = routes.at[:, pl.ds(1, ring - 1)]
            return pltpu.make_async_remote_copy(
                src_ref=ref, dst_ref=ref, send_sem=route_out.at[0], recv_sem=route_in.at[0],
                device_id=ring_peer(0, 1), device_id_type=MESH_ID)

        def near_step(way):
            return 1 if way == 0 else ring - 1

        def relay_part(way):
            return pl.ds(way * mid, mid)

        def own_part(way):
            return pl.ds((1 - way) * mid, mid)

        def far_copy(h, q, way):
            return pltpu.make_async_remote_copy(
                src_ref=far_out.at[h, q, way], dst_ref=far_in.at[h, q, way],
                send_sem=far_sent.at[0], recv_sem=far_here.at[h, q, way],
                device_id=ring_peer(h, near_step(way)), device_id_type=MESH_ID)

        def own_copy(h, q, way):
            return pltpu.make_async_remote_copy(
                src_ref=near_out.at[h, q, way, own_part(way)], dst_ref=near_in.at[h, q, way, own_part(way)],
                send_sem=near_sent.at[0], recv_sem=own_here.at[h, q],
                device_id=ring_peer(h, near_step(way)), device_id_type=MESH_ID)

        def sum_copy(h, q, way):
            return pltpu.make_async_remote_copy(
                src_ref=near_out.at[h, q, way, relay_part(way)], dst_ref=near_in.at[h, q, way, relay_part(way)],
                send_sem=near_sent.at[0], recv_sem=sum_here.at[h, q],
                device_id=ring_peer(h, near_step(way)), device_id_type=MESH_ID)

        def both_ways(h, q, here):
            return whole(near_in.at[h, q, :, pl.ds(0, mid)], near_sent.at[0], here.at[h, q])

        def part_copies(k):
            cols = pl.ds(k * k_size, k_size)
            return (pltpu.make_async_copy(x_hbm.at[:, 0, :, cols], x_buf.at[0, :, :, cols], part_sem.at[0, k]),
                    pltpu.make_async_copy(wg_hbm.at[0, cols], wg_buf.at[0, cols], part_sem.at[1, k]),
                    pltpu.make_async_copy(wu_hbm.at[0, cols], wu_buf.at[0, cols], part_sem.at[2, k]))

        def down_part_copy(h, q):
            cols = pl.ds(h * half + q * quarter, quarter)
            return pltpu.make_async_copy(wd_hbm.at[0, :, cols], wd_buf.at[0, :, cols], down_sem.at[h, q])

        def weight_copies(e):
            slot = lax.rem(e, WEIGHT_SLOTS)
            return (pltpu.make_async_copy(x_hbm.at[:, e], x_buf.at[slot], weight_sem.at[0, e - 1]),
                    pltpu.make_async_copy(wg_hbm.at[e], wg_buf.at[slot], weight_sem.at[1, e - 1]),
                    pltpu.make_async_copy(wu_hbm.at[e], wu_buf.at[slot], weight_sem.at[2, e - 1]),
                    pltpu.make_async_copy(wd_hbm.at[e], wd_buf.at[slot], weight_sem.at[3, e - 1]))

        def token_copies():
            return (pltpu.make_async_copy(slot_hbm, slot_buf, token_sem.at[0]),
                    pltpu.make_async_copy(eid_hbm, eid_buf, token_sem.at[1]),
                    pltpu.make_async_copy(gate_hbm, gate_buf, token_sem.at[2]))

        for k in range(K_PARTS):
            for copy in part_copies(k):
                copy.start()
        greet = [first_peer(h, step, flip)[0] for h in range(HALVES) for step, flip in hops[:-1]] + [first_peer(0, 0, 1)[0]]
        barrier = pltpu.get_barrier_semaphore()
        for peer in greet:
            pl.semaphore_signal(barrier, inc=1, device_id=peer, device_id_type=MESH_ID)
        for h, q in blocks:
            down_part_copy(h, q).start()
        for copy in token_copies():
            copy.start()
        for copy in weight_copies(1):
            copy.start()

        def first_send(h, q, e):
            for step, flip in hops:
                first_copy(h, e, q, step, flip).start()

        def keep_own(h, e):
            cols = pl.ds(h * half, half)
            if h == 0:
                recv_buf[h, e, source[h]] = send_buf[e, :, chip, core, :, cols]
            else:
                recv_buf[h, e, source[h]] = send_buf[e, row, :, core, :, cols]

        def activation(gate_proj, up_proj):
            return (jax.nn.silu(gate_proj) * up_proj).astype(jnp.bfloat16)

        def down_step(e, slot, start, size, hidden):
            cols = pl.ds(start, size)
            y = jnp.dot(hidden, wd_buf[slot, :, cols], preferred_element_type=jnp.float32)
            send_buf[e, :, :, :, :, cols] = y.reshape(ring, ring, CORES, capacity, size).astype(jnp.bfloat16)

        gate_proj = up_proj = None
        for k in range(K_PARTS):
            for copy in part_copies(k):
                copy.wait()
            cols = pl.ds(k * k_size, k_size)
            x_rows = x_buf[0, :, :, cols].reshape(rows, k_size)
            gate_part = jnp.dot(x_rows, wg_buf[0, cols], preferred_element_type=jnp.float32)
            up_part = jnp.dot(x_rows, wu_buf[0, cols], preferred_element_type=jnp.float32)
            gate_proj = gate_part if gate_proj is None else gate_proj + gate_part
            up_proj = up_part if up_proj is None else up_proj + up_part
        hidden = activation(gate_proj, up_proj)
        for h, q in blocks:
            down_part_copy(h, q).wait()
            down_step(0, 0, h * half + q * quarter, quarter, hidden)
            if (h, q) == blocks[0]:
                pl.semaphore_wait(barrier, len(greet))
            if (h, q) == blocks[0]:
                for copy in weight_copies(2):
                    copy.start()
            first_send(h, q, 0)
        for h in range(HALVES):
            keep_own(h, 0)

        for copy in token_copies():
            copy.wait()
        slots = slot_buf[...]
        keys = jnp.where(slots >= 0, eid_buf[...] * capacity + slots, -1).astype(jnp.float32)
        for h in range(HALVES):
            routes[h, 0, 0:top] = keys
            routes[h, 0, top:2 * top] = gate_buf[...]
        for h in range(HALVES):
            for step in range(1, ring):
                route_copy(h, step).start()

        @pl.loop(1, experts)
        def _(e):
            slot = lax.rem(e, WEIGHT_SLOTS)
            x_copy, gate_copy, up_copy, down_copy = weight_copies(e)
            x_copy.wait()
            x_rows = x_buf[slot].reshape(rows, width)
            gate_copy.wait()
            gate_proj = jnp.dot(x_rows, wg_buf[slot], preferred_element_type=jnp.float32)
            up_copy.wait()
            up_proj = jnp.dot(x_rows, wu_buf[slot], preferred_element_type=jnp.float32)
            hidden = activation(gate_proj, up_proj)
            down_copy.wait()

            @pl.when(e + 2 < experts)
            def _():
                for copy in weight_copies(e + 2):
                    copy.start()
            for h in range(HALVES):
                down_step(e, slot, h * half, half, hidden)
                for q in range(QUARTERS):
                    first_send(h, q, e)
            for h in range(HALVES):
                keep_own(h, e)

        route_all().wait_recv()
        line = lax.broadcasted_iota(jnp.int32, (part_rows, tokens), 0)
        local = line // (peers * capacity)
        src = lax.rem(line // capacity, peers)
        device = (row * peers + src, (src // CORES) * peers + chip * CORES + lax.rem(src, CORES))
        for h in range(HALVES):
            row_key = ((device[h] * experts + local) * capacity + lax.rem(line, capacity)).astype(jnp.float32)
            for step in range(ring):
                weight = jnp.zeros((part_rows, tokens), jnp.float32)
                for j in range(top):
                    weight = weight + jnp.where(row_key == routes[h, step, j:j + 1], routes[h, step, top + j:top + j + 1], 0.0)
                used_buf[h, step] = jnp.broadcast_to(jnp.max(weight, axis=1, keepdims=True), (part_rows, 128))
                weight = weight.T
                high = jnp.minimum(weight, BF16_MAX).astype(jnp.bfloat16)
                rest = weight - high.astype(jnp.float32)
                middle = rest.astype(jnp.bfloat16)
                low = (rest - middle.astype(jnp.float32)).astype(jnp.bfloat16)
                w_buf[h, step, 0:tokens] = high
                w_buf[h, step, tokens:2 * tokens] = middle
                w_buf[h, step, 2 * tokens:3 * tokens] = low

        def partial(h, q, step):
            y = recv_buf[h, :, :, shift(place[h], step), :, pl.ds(q * quarter, quarter)]
            y = y.astype(jnp.float32).reshape(part_rows, quarter)
            used = used_buf[h, step] > 0.0
            y = jnp.where(jnp.concatenate([used] * (quarter // 128), axis=1), y, 0.0).astype(jnp.bfloat16)
            part = jnp.dot(w_buf[h, step], y, preferred_element_type=jnp.float32)
            return part[0:tokens] + (part[tokens:2 * tokens] + part[2 * tokens:3 * tokens])

        late_core = core == 0
        for h, q in blocks:
            first_here(h, q).wait_recv()
            far = partial(h, q, 2)
            for way in range(2):
                far_out[h, q, way] = far[way * mid:(way + 1) * mid]
                far_copy(h, q, way).start()
            for way in range(2):
                near_out[h, q, way] = partial(h, q, near_step(way))

            @pl.when(jnp.logical_not(late_core))
            def _():
                for way in range(2):
                    own_copy(h, q, way).start()
        for h, q in blocks:
            for way in range(2):
                far_copy(h, q, way).wait_recv()
                near_out[h, q, way, relay_part(way)] = near_out[h, q, way, relay_part(way)] + far_in[h, q, way]
                sum_copy(h, q, way).start()
            acc[:, pl.ds(h * half + q * quarter, quarter)] = partial(h, q, 0)
        for h, q in blocks:
            both_ways(h, q, sum_here).wait_recv()

            if q == QUARTERS - 1:
                @pl.when(late_core)
                def _():
                    for part in range(QUARTERS):
                        for way in range(2):
                            own_copy(h, part, way).start()
        for h, q in blocks:
            both_ways(h, q, own_here).wait_recv()
            cols = pl.ds(h * half + q * quarter, quarter)
            out_ref[:, cols] = (acc[:, cols] + near_in[h, q, 0] + near_in[h, q, 1]).astype(jnp.bfloat16)

        route_all().wait_send()
        first_sent().wait_send()
        whole(far_out, far_sent.at[0], far_here.at[0, 0, 0]).wait_send()
        whole(near_out, near_sent.at[0], own_here.at[0, 0]).wait_send()

    return kernel


def solution(mesh):
    outer_devs = mesh.shape["outer"]
    inner_devs = mesh.shape["expert"]
    assert inner_devs == outer_devs * CORES and outer_devs == 4

    def local_step(x_disp, w_gate, w_up, w_down, slot_idx, expert_ids, gate_wts):
        group, experts, capacity, width = x_disp.shape
        ff = w_gate.shape[2]
        tokens, top = slot_idx.shape
        rows = group * capacity
        ring = outer_devs
        peers = inner_devs
        half = width // HALVES
        quarter = half // QUARTERS
        bf16, f32 = jnp.bfloat16, jnp.float32
        hbm = pl.BlockSpec(memory_space=pltpu.HBM)
        dma = pltpu.SemaphoreType.DMA
        return pl.pallas_call(
            make_kernel(ring, experts, capacity, width, ff, tokens, top),
            out_shape=pltpu.VMEM((tokens, width), bf16),
            in_specs=[hbm] * 7,
            out_specs=pl.BlockSpec(memory_space=pltpu.VMEM),
            scratch_shapes=[
                pltpu.VMEM((WEIGHT_SLOTS, group, capacity, width), bf16),
                pltpu.VMEM((WEIGHT_SLOTS, width, ff), bf16),
                pltpu.VMEM((WEIGHT_SLOTS, width, ff), bf16),
                pltpu.VMEM((WEIGHT_SLOTS, ff, width), bf16),
                pltpu.VMEM((top, tokens), jnp.int32),
                pltpu.VMEM((top, tokens), jnp.int32),
                pltpu.VMEM((top, tokens), f32),
                pltpu.VMEM((experts, ring, ring, CORES, capacity, width), bf16),
                pltpu.VMEM((HALVES, experts, peers, ring, capacity, half), bf16),
                pltpu.VMEM((HALVES, ring, 2 * top, tokens), f32),
                pltpu.VMEM((HALVES, ring, 3 * tokens, experts * peers * capacity), bf16),
                pltpu.VMEM((HALVES, ring, experts * peers * capacity, 128), f32),
                pltpu.VMEM((HALVES, QUARTERS, 2, tokens // 2, quarter), f32),
                pltpu.VMEM((HALVES, QUARTERS, 2, tokens // 2, quarter), f32),
                pltpu.VMEM((HALVES, QUARTERS, 2, tokens, quarter), f32),
                pltpu.VMEM((HALVES, QUARTERS, 2, tokens, quarter), f32),
                pltpu.VMEM((tokens, width), f32),
                dma((3, K_PARTS)),
                dma((HALVES, QUARTERS)),
                dma((4, experts - 1)),
                dma((3,)),
                dma((1,)),
                dma((HALVES, QUARTERS)),
                dma((1,)),
                dma((1,)),
                dma((1,)),
                dma((HALVES, QUARTERS, 2)),
                dma((1,)),
                dma((HALVES, QUARTERS)),
                dma((HALVES, QUARTERS)),
            ],
            compiler_params=pltpu.CompilerParams(collective_id=0, has_side_effects=True, vmem_limit_bytes=VMEM_LIMIT),
        )(x_disp, w_gate, w_up, w_down, slot_idx.T, expert_ids.T, gate_wts.T)

    expert_spec = P(("outer", "expert"))
    token_spec = P(("data", "outer", "expert"))
    return jax.shard_map(local_step, mesh=mesh, in_specs=(P("data", ("outer", "expert")), expert_spec, expert_spec, expert_spec, token_spec, token_spec, token_spec), out_specs=token_spec, check_vma=False)
```

```python
import jax
import jax.numpy as jnp
from jax import lax
from jax.experimental import pallas as pl
from jax.experimental.pallas import tpu as pltpu
from jax.sharding import PartitionSpec as P

MESH_ID = pl.DeviceIdType.MESH
CORES = 2
BLOCKS = ((0, 0, 512), (1, 1024, 512), (0, 512, 512), (1, 1536, 512))
LATE = ((1, 0), (1, 1), (2, 2), (3, 3))
HALVES = 2
DOWN_PARTS = 2
K_SIZES = (512, 512, 512, 512)
K_PARTS = len(K_SIZES)
FIRST_ORDER = (0, 1, 2, 3)
WEIGHT_SLOTS = 3
VMEM_LIMIT = 62 * 2 ** 20
BF16_MAX = 3.3895313892515355e38


def make_kernel(ring, experts, capacity, width, ff, tokens, top):
    peers = ring * CORES
    group = ring * peers
    rows = group * capacity
    part_rows = experts * peers * capacity
    n_blocks = len(BLOCKS)
    down_size = width // DOWN_PARTS
    mid = tokens // 2

    def kernel(x_hbm, wg_hbm, wu_hbm, wd_hbm, slot_hbm, eid_hbm, gate_hbm, out_ref,
               x_buf, wg_buf, wu_buf, wd_buf, slot_buf, eid_buf, gate_buf, send_buf, recv_buf,
               routes, w_buf, used_buf, far_out, far_in, near_out, near_in, acc,
               part_sem, down_sem, weight_sem, token_sem, first_out, first_in, route_out, route_in,
               far_sent, far_here, near_sent, own_here, sum_here):
        row = lax.axis_index("outer")
        col = lax.axis_index("expert")
        chip, core = col // CORES, lax.rem(col, CORES)
        def columns(b):
            return pl.ds(BLOCKS[b][1], BLOCKS[b][2])

        place = (row, chip)
        source = (col, row * CORES + core)

        def shift(start, step):
            return lax.rem(start + step, ring)

        def ring_peer(h, step):
            if h == 0:
                return {"outer": shift(row, step), "expert": col}
            return {"outer": row, "expert": shift(chip, step) * CORES + core}

        def first_peer(h, step, flip):
            other = lax.rem(core + flip, CORES)
            if h == 0:
                to = shift(chip, step)
                return {"outer": row, "expert": to * CORES + other}, to, other
            to = shift(row, step)
            return {"outer": to, "expert": chip * CORES + other}, to, other

        def rows_for(h, e, to, other, cols):
            if h == 0:
                return send_buf.at[e, :, to, other, :, cols]
            return send_buf.at[e, to, :, other, :, cols]

        hops = [(2, 0), (2, 1), (1, 0), (ring - 1, 0), (1, 1), (ring - 1, 1), (0, 1)]

        def first_copy(b, e, step, flip):
            h = BLOCKS[b][0]
            peer, to, other = first_peer(h, step, flip)
            return pltpu.make_async_remote_copy(
                src_ref=rows_for(h, e, to, other, columns(b)),
                dst_ref=recv_buf.at[e, source[h], :, :, columns(b)],
                send_sem=first_out.at[0], recv_sem=first_in.at[b],
                device_id=peer, device_id_type=MESH_ID)

        def whole(ref, sent, here):
            return pltpu.make_async_remote_copy(
                src_ref=ref, dst_ref=ref, send_sem=sent, recv_sem=here,
                device_id=ring_peer(0, 1), device_id_type=MESH_ID)

        def first_here(b):
            return whole(recv_buf.at[:, pl.ds(0, peers - 1), :, :, columns(b)], first_out.at[0], first_in.at[b])

        def first_sent():
            return whole(recv_buf.at[:, pl.ds(0, peers - 1)], first_out.at[0], first_in.at[0])

        def route_copy(h, step):
            return pltpu.make_async_remote_copy(
                src_ref=routes.at[h, 0], dst_ref=routes.at[h, ring - step],
                send_sem=route_out.at[0], recv_sem=route_in.at[0],
                device_id=ring_peer(h, step), device_id_type=MESH_ID)

        def route_all():
            ref = routes.at[:, pl.ds(1, ring - 1)]
            return pltpu.make_async_remote_copy(
                src_ref=ref, dst_ref=ref, send_sem=route_out.at[0], recv_sem=route_in.at[0],
                device_id=ring_peer(0, 1), device_id_type=MESH_ID)

        def near_step(way):
            return 1 if way == 0 else ring - 1

        def relay_part(way):
            return pl.ds(way * mid, mid)

        def own_part(way):
            return pl.ds((1 - way) * mid, mid)

        def ring_copy(b, way, src, dst, sent, here):
            return pltpu.make_async_remote_copy(
                src_ref=src, dst_ref=dst, send_sem=sent.at[0], recv_sem=here,
                device_id=ring_peer(BLOCKS[b][0], near_step(way)), device_id_type=MESH_ID)

        def far_copy(b, way):
            cols = columns(b)
            return ring_copy(b, way, far_out.at[way, :, cols], far_in.at[way, :, cols], far_sent, far_here.at[b, way])

        def own_copy(b, way):
            cols, part = columns(b), own_part(way)
            return ring_copy(b, way, near_out.at[way, part, cols], near_in.at[way, part, cols], near_sent, own_here.at[b])

        def sum_copy(b, way):
            cols, part = columns(b), relay_part(way)
            return ring_copy(b, way, near_out.at[way, part, cols], near_in.at[way, part, cols], near_sent, sum_here.at[b])

        def both_ways(b, here):
            return whole(near_in.at[:, pl.ds(0, mid), columns(b)], near_sent.at[0], here.at[b])

        def k_slice(k):
            return pl.ds(sum(K_SIZES[:k]), K_SIZES[k])

        def part_copies(k):
            cols = k_slice(k)
            return (pltpu.make_async_copy(x_hbm.at[:, 0, :, cols], x_buf.at[0, :, :, cols], part_sem.at[0, k]),
                    pltpu.make_async_copy(wg_hbm.at[0, cols], wg_buf.at[0, cols], part_sem.at[1, k]),
                    pltpu.make_async_copy(wu_hbm.at[0, cols], wu_buf.at[0, cols], part_sem.at[2, k]))

        def down_part_copy(b):
            cols = columns(b)
            return pltpu.make_async_copy(wd_hbm.at[0, :, cols], wd_buf.at[0, :, cols], down_sem.at[b])

        def weight_copies(e):
            slot = lax.rem(e, WEIGHT_SLOTS)
            return (pltpu.make_async_copy(x_hbm.at[:, e], x_buf.at[slot], weight_sem.at[0, lax.rem(e, 2)]),
                    pltpu.make_async_copy(wg_hbm.at[e], wg_buf.at[slot], weight_sem.at[1, lax.rem(e, 2)]),
                    pltpu.make_async_copy(wu_hbm.at[e], wu_buf.at[slot], weight_sem.at[2, lax.rem(e, 2)]),
                    pltpu.make_async_copy(wd_hbm.at[e], wd_buf.at[slot], weight_sem.at[3, lax.rem(e, 2)]))

        def token_copies():
            return (pltpu.make_async_copy(slot_hbm, slot_buf, token_sem.at[0]),
                    pltpu.make_async_copy(eid_hbm, eid_buf, token_sem.at[1]),
                    pltpu.make_async_copy(gate_hbm, gate_buf, token_sem.at[2]))

        for k in range(K_PARTS):
            for copy in part_copies(k):
                copy.start()
        greet = [first_peer(h, step, flip)[0] for h in range(HALVES) for step, flip in hops[:-1]] + [first_peer(0, 0, 1)[0]]
        barrier = pltpu.get_barrier_semaphore()
        for peer in greet:
            pl.semaphore_signal(barrier, inc=1, device_id=peer, device_id_type=MESH_ID)
        for b in FIRST_ORDER:
            down_part_copy(b).start()
        for copy in token_copies():
            copy.start()
        for copy in weight_copies(1):
            copy.start()

        def first_send(b, e):
            for step, flip in hops:
                first_copy(b, e, step, flip).start()

        def keep_own(e):
            for b in range(n_blocks):
                cols = columns(b)
                if BLOCKS[b][0] == 0:
                    recv_buf[e, source[0], :, :, cols] = send_buf[e, :, chip, core, :, cols]
                else:
                    recv_buf[e, source[1], :, :, cols] = send_buf[e, row, :, core, :, cols]

        def activation(gate_proj, up_proj):
            return (jax.nn.silu(gate_proj) * up_proj).astype(jnp.bfloat16)

        def down_step(e, slot, start, size, hidden):
            cols = pl.ds(start, size)
            y = jnp.dot(hidden, wd_buf[slot, :, cols], preferred_element_type=jnp.float32)
            send_buf[e, :, :, :, :, cols] = y.reshape(ring, ring, CORES, capacity, size).astype(jnp.bfloat16)

        gate_proj = up_proj = None
        for k in range(K_PARTS):
            for copy in part_copies(k):
                copy.wait()
            cols = k_slice(k)
            x_rows = x_buf[0, :, :, cols].reshape(rows, K_SIZES[k])
            gate_part = jnp.dot(x_rows, wg_buf[0, cols], preferred_element_type=jnp.float32)
            up_part = jnp.dot(x_rows, wu_buf[0, cols], preferred_element_type=jnp.float32)
            gate_proj = gate_part if gate_proj is None else gate_proj + gate_part
            up_proj = up_part if up_proj is None else up_proj + up_part
        hidden = activation(gate_proj, up_proj)
        for b in FIRST_ORDER:
            down_part_copy(b).wait()
            down_step(0, 0, BLOCKS[b][1], BLOCKS[b][2], hidden)
            if b == FIRST_ORDER[0]:
                pl.semaphore_wait(barrier, len(greet))
                for copy in weight_copies(2):
                    copy.start()
            first_send(b, 0)
        keep_own(0)

        for copy in token_copies():
            copy.wait()
        slots = slot_buf[...]
        keys = jnp.where(slots >= 0, eid_buf[...] * capacity + slots, -1).astype(jnp.float32)
        for h in range(HALVES):
            routes[h, 0, 0:top] = keys
            routes[h, 0, top:2 * top] = gate_buf[...]
        for h in range(HALVES):
            for step in range(1, ring):
                route_copy(h, step).start()

        @pl.loop(1, experts)
        def _(e):
            slot = lax.rem(e, WEIGHT_SLOTS)
            x_copy, gate_copy, up_copy, down_copy = weight_copies(e)
            x_copy.wait()
            x_rows = x_buf[slot].reshape(rows, width)
            gate_copy.wait()
            gate_proj = jnp.dot(x_rows, wg_buf[slot], preferred_element_type=jnp.float32)
            up_copy.wait()
            up_proj = jnp.dot(x_rows, wu_buf[slot], preferred_element_type=jnp.float32)
            hidden = activation(gate_proj, up_proj)
            down_copy.wait()

            @pl.when(e + 2 < experts)
            def _():
                for copy in weight_copies(e + 2):
                    copy.start()
            for part in range(DOWN_PARTS):
                down_step(e, slot, part * down_size, down_size, hidden)
                for b in range(n_blocks // 2):
                    if (BLOCKS[b][1] + BLOCKS[b][2] - 1) // down_size == part:
                        first_send(b, e)

            @pl.when(e == experts - 1)
            def _():
                for b in range(n_blocks // 2, n_blocks):
                    first_send(b, e - 1)

            @pl.when(e != experts - 2)
            def _():
                for b in range(n_blocks // 2, n_blocks):
                    first_send(b, e)
            keep_own(e)

        route_all().wait_recv()
        line = lax.broadcasted_iota(jnp.int32, (part_rows, tokens), 0)
        local = line // (peers * capacity)
        src = lax.rem(line // capacity, peers)
        device = (row * peers + src, (src // CORES) * peers + chip * CORES + lax.rem(src, CORES))
        for h in range(HALVES):
            row_key = ((device[h] * experts + local) * capacity + lax.rem(line, capacity)).astype(jnp.float32)
            for step in range(ring):
                weight = jnp.zeros((part_rows, tokens), jnp.float32)
                for j in range(top):
                    weight = weight + jnp.where(row_key == routes[h, step, j:j + 1], routes[h, step, top + j:top + j + 1], 0.0)
                used_buf[h, step] = jnp.broadcast_to(jnp.max(weight, axis=1, keepdims=True), (part_rows, 128))
                weight = weight.T
                high = jnp.minimum(weight, BF16_MAX).astype(jnp.bfloat16)
                rest = weight - high.astype(jnp.float32)
                middle = rest.astype(jnp.bfloat16)
                low = (rest - middle.astype(jnp.float32)).astype(jnp.bfloat16)
                w_buf[h, step, 0:tokens] = high
                w_buf[h, step, tokens:2 * tokens] = middle
                w_buf[h, step, 2 * tokens:3 * tokens] = low

        def partial(b, step):
            h, _, size = BLOCKS[b]
            y = recv_buf[:, :, shift(place[h], step), :, columns(b)]
            y = y.astype(jnp.float32).reshape(part_rows, size)
            used = used_buf[h, step] > 0.0
            y = jnp.where(jnp.concatenate([used] * (size // 128), axis=1), y, 0.0).astype(jnp.bfloat16)
            part = jnp.dot(w_buf[h, step], y, preferred_element_type=jnp.float32)
            return part[0:tokens] + (part[tokens:2 * tokens] + part[2 * tokens:3 * tokens])

        late_core = core == 0
        for b in range(n_blocks):
            first_here(b).wait_recv()
            far = partial(b, 2)
            for way in range(2):
                far_out[way, :, columns(b)] = far[way * mid:(way + 1) * mid]
                far_copy(b, way).start()
            for way in range(2):
                near_out[way, :, columns(b)] = partial(b, near_step(way))

            @pl.when(jnp.logical_not(late_core))
            def _():
                for way in range(2):
                    own_copy(b, way).start()
        for b in range(n_blocks):
            for way in range(2):
                far_copy(b, way).wait_recv()
                part, cols = relay_part(way), columns(b)
                near_out[way, part, cols] = near_out[way, part, cols] + far_in[way, :, cols]
                sum_copy(b, way).start()
            acc[:, columns(b)] = partial(b, 0)
        for b in range(n_blocks):
            both_ways(b, sum_here).wait_recv()
            late = [n for trigger, n in LATE if trigger == b]
            if late:
                @pl.when(late_core)
                def _():
                    for n in late:
                        for way in range(2):
                            own_copy(n, way).start()
        for b in range(n_blocks):
            both_ways(b, own_here).wait_recv()
            cols = columns(b)
            out_ref[:, cols] = (acc[:, cols] + near_in[0, :, cols] + near_in[1, :, cols]).astype(jnp.bfloat16)

        route_all().wait_send()
        first_sent().wait_send()
        whole(far_out, far_sent.at[0], far_here.at[0, 0]).wait_send()
        whole(near_out, near_sent.at[0], own_here.at[0]).wait_send()

    return kernel


def solution(mesh):
    outer_devs = mesh.shape["outer"]
    inner_devs = mesh.shape["expert"]
    assert inner_devs == outer_devs * CORES and outer_devs == 4

    def local_step(x_disp, w_gate, w_up, w_down, slot_idx, expert_ids, gate_wts):
        group, experts, capacity, width = x_disp.shape
        ff = w_gate.shape[2]
        tokens, top = slot_idx.shape
        rows = group * capacity
        ring = outer_devs
        peers = inner_devs
        n_blocks = len(BLOCKS)
        bf16, f32 = jnp.bfloat16, jnp.float32
        hbm = pl.BlockSpec(memory_space=pltpu.HBM)
        dma = pltpu.SemaphoreType.DMA
        return pl.pallas_call(
            make_kernel(ring, experts, capacity, width, ff, tokens, top),
            out_shape=pltpu.VMEM((tokens, width), bf16),
            in_specs=[hbm] * 7,
            out_specs=pl.BlockSpec(memory_space=pltpu.VMEM),
            scratch_shapes=[
                pltpu.VMEM((WEIGHT_SLOTS, group, capacity, width), bf16),
                pltpu.VMEM((WEIGHT_SLOTS, width, ff), bf16),
                pltpu.VMEM((WEIGHT_SLOTS, width, ff), bf16),
                pltpu.VMEM((WEIGHT_SLOTS, ff, width), bf16),
                pltpu.VMEM((top, tokens), jnp.int32),
                pltpu.VMEM((top, tokens), jnp.int32),
                pltpu.VMEM((top, tokens), f32),
                pltpu.VMEM((experts, ring, ring, CORES, capacity, width), bf16),
                pltpu.VMEM((experts, peers, ring, capacity, width), bf16),
                pltpu.VMEM((HALVES, ring, 2 * top, tokens), f32),
                pltpu.VMEM((HALVES, ring, 3 * tokens, experts * peers * capacity), bf16),
                pltpu.VMEM((HALVES, ring, experts * peers * capacity, 128), f32),
                pltpu.VMEM((2, tokens // 2, width), f32),
                pltpu.VMEM((2, tokens // 2, width), f32),
                pltpu.VMEM((2, tokens, width), f32),
                pltpu.VMEM((2, tokens, width), f32),
                pltpu.VMEM((tokens, width), f32),
                dma((3, K_PARTS)),
                dma((n_blocks,)),
                dma((4, 2)),
                dma((3,)),
                dma((1,)),
                dma((n_blocks,)),
                dma((1,)),
                dma((1,)),
                dma((1,)),
                dma((n_blocks, 2)),
                dma((1,)),
                dma((n_blocks,)),
                dma((n_blocks,)),
            ],
            compiler_params=pltpu.CompilerParams(collective_id=0, has_side_effects=True, vmem_limit_bytes=VMEM_LIMIT),
        )(x_disp, w_gate, w_up, w_down, slot_idx.T, expert_ids.T, gate_wts.T)

    expert_spec = P(("outer", "expert"))
    token_spec = P(("data", "outer", "expert"))
    return jax.shard_map(local_step, mesh=mesh, in_specs=(P("data", ("outer", "expert")), expert_spec, expert_spec, expert_spec, token_spec, token_spec, token_spec), out_specs=token_spec, check_vma=False)
```

```python
import jax
import jax.numpy as jnp
from jax import lax
from jax.experimental import pallas as pl
from jax.experimental.pallas import tpu as pltpu
from jax.sharding import PartitionSpec as P

MESH_ID = pl.DeviceIdType.MESH
CORES = 2
BLOCKS = ((0, 0, 512), (1, 1024, 512), (0, 512, 512), (1, 1536, 512))
LATE = ((0, 0), (0, 1), (0, 2), (0, 3))
HALVES = 2
DOWN_PARTS = 2
K_SIZES = (512, 512, 512, 512)
K_PARTS = len(K_SIZES)
FIRST_ORDER = (1, 0, 3, 2)
WEIGHT_SLOTS = 3
VMEM_LIMIT = 62 * 2 ** 20
BF16_MAX = 3.3895313892515355e38


def make_kernel(ring, experts, capacity, width, ff, tokens, top):
    peers = ring * CORES
    group = ring * peers
    rows = group * capacity
    part_rows = experts * peers * capacity
    n_blocks = len(BLOCKS)
    down_size = width // DOWN_PARTS
    mid = tokens // 2

    def kernel(x_hbm, wg_hbm, wu_hbm, wd_hbm, slot_hbm, eid_hbm, gate_hbm, out_ref,
               x_buf, wg_buf, wu_buf, wd_buf, slot_buf, eid_buf, gate_buf, send_buf, recv_buf,
               routes, w_buf, used_buf, far_out, far_in, near_out, near_in, acc,
               part_sem, down_sem, weight_sem, token_sem, first_out, first_in, route_out, route_in,
               far_sent, far_here, near_sent, own_here, sum_here):
        row = lax.axis_index("outer")
        col = lax.axis_index("expert")
        chip, core = col // CORES, lax.rem(col, CORES)
        def columns(b):
            return pl.ds(BLOCKS[b][1], BLOCKS[b][2])

        place = (row, chip)
        source = (col, row * CORES + core)

        def shift(start, step):
            return lax.rem(start + step, ring)

        def ring_peer(h, step):
            if h == 0:
                return {"outer": shift(row, step), "expert": col}
            return {"outer": row, "expert": shift(chip, step) * CORES + core}

        def first_peer(h, step, flip):
            other = lax.rem(core + flip, CORES)
            if h == 0:
                to = shift(chip, step)
                return {"outer": row, "expert": to * CORES + other}, to, other
            to = shift(row, step)
            return {"outer": to, "expert": chip * CORES + other}, to, other

        def rows_for(h, e, to, other, cols):
            if h == 0:
                return send_buf.at[e, :, to, other, :, cols]
            return send_buf.at[e, to, :, other, :, cols]

        hops = [(2, 0), (2, 1), (1, 0), (ring - 1, 0), (1, 1), (ring - 1, 1), (0, 1)]

        def first_copy(b, e, step, flip):
            h = BLOCKS[b][0]
            peer, to, other = first_peer(h, step, flip)
            return pltpu.make_async_remote_copy(
                src_ref=rows_for(h, e, to, other, columns(b)),
                dst_ref=recv_buf.at[e, source[h], :, :, columns(b)],
                send_sem=first_out.at[0], recv_sem=first_in.at[b],
                device_id=peer, device_id_type=MESH_ID)

        def whole(ref, sent, here):
            return pltpu.make_async_remote_copy(
                src_ref=ref, dst_ref=ref, send_sem=sent, recv_sem=here,
                device_id=ring_peer(0, 1), device_id_type=MESH_ID)

        def first_here(b):
            return whole(recv_buf.at[:, pl.ds(0, peers - 1), :, :, columns(b)], first_out.at[0], first_in.at[b])

        def first_sent():
            return whole(recv_buf.at[:, pl.ds(0, peers - 1)], first_out.at[0], first_in.at[0])

        def route_copy(h, step):
            return pltpu.make_async_remote_copy(
                src_ref=routes.at[h, 0], dst_ref=routes.at[h, ring - step],
                send_sem=route_out.at[0], recv_sem=route_in.at[0],
                device_id=ring_peer(h, step), device_id_type=MESH_ID)

        def route_all():
            ref = routes.at[:, pl.ds(1, ring - 1)]
            return pltpu.make_async_remote_copy(
                src_ref=ref, dst_ref=ref, send_sem=route_out.at[0], recv_sem=route_in.at[0],
                device_id=ring_peer(0, 1), device_id_type=MESH_ID)

        def near_step(way):
            return 1 if way == 0 else ring - 1

        def relay_part(way):
            return pl.ds(way * mid, mid)

        def own_part(way):
            return pl.ds((1 - way) * mid, mid)

        def ring_copy(b, way, src, dst, sent, here):
            return pltpu.make_async_remote_copy(
                src_ref=src, dst_ref=dst, send_sem=sent.at[0], recv_sem=here,
                device_id=ring_peer(BLOCKS[b][0], near_step(way)), device_id_type=MESH_ID)

        def far_copy(b, way):
            cols = columns(b)
            return ring_copy(b, way, far_out.at[way, :, cols], far_in.at[way, :, cols], far_sent, far_here.at[b, way])

        def own_copy(b, way):
            cols, part = columns(b), own_part(way)
            return ring_copy(b, way, near_out.at[way, part, cols], near_in.at[way, part, cols], near_sent, own_here.at[b])

        def sum_copy(b, way):
            cols, part = columns(b), relay_part(way)
            return ring_copy(b, way, near_out.at[way, part, cols], near_in.at[way, part, cols], near_sent, sum_here.at[b])

        def both_ways(b, here):
            return whole(near_in.at[:, pl.ds(0, mid), columns(b)], near_sent.at[0], here.at[b])

        def k_slice(k):
            return pl.ds(sum(K_SIZES[:k]), K_SIZES[k])

        def part_copies(k):
            cols = k_slice(k)
            return (pltpu.make_async_copy(x_hbm.at[:, 0, :, cols], x_buf.at[0, :, :, cols], part_sem.at[0, k]),
                    pltpu.make_async_copy(wg_hbm.at[0, cols], wg_buf.at[0, cols], part_sem.at[1, k]),
                    pltpu.make_async_copy(wu_hbm.at[0, cols], wu_buf.at[0, cols], part_sem.at[2, k]))

        def down_part_copy(b):
            cols = columns(b)
            return pltpu.make_async_copy(wd_hbm.at[0, :, cols], wd_buf.at[0, :, cols], down_sem.at[b])

        def weight_copies(e):
            slot = lax.rem(e, WEIGHT_SLOTS)
            return (pltpu.make_async_copy(x_hbm.at[:, e], x_buf.at[slot], weight_sem.at[0, lax.rem(e, 2)]),
                    pltpu.make_async_copy(wg_hbm.at[e], wg_buf.at[slot], weight_sem.at[1, lax.rem(e, 2)]),
                    pltpu.make_async_copy(wu_hbm.at[e], wu_buf.at[slot], weight_sem.at[2, lax.rem(e, 2)]),
                    pltpu.make_async_copy(wd_hbm.at[e], wd_buf.at[slot], weight_sem.at[3, lax.rem(e, 2)]))

        def token_copies():
            return (pltpu.make_async_copy(slot_hbm, slot_buf, token_sem.at[0]),
                    pltpu.make_async_copy(eid_hbm, eid_buf, token_sem.at[1]),
                    pltpu.make_async_copy(gate_hbm, gate_buf, token_sem.at[2]))

        for k in range(K_PARTS):
            for copy in part_copies(k):
                copy.start()
        greet = [first_peer(h, step, flip)[0] for h in range(HALVES) for step, flip in hops[:-1]] + [first_peer(0, 0, 1)[0]]
        barrier = pltpu.get_barrier_semaphore()
        for peer in greet:
            pl.semaphore_signal(barrier, inc=1, device_id=peer, device_id_type=MESH_ID)
        for b in FIRST_ORDER:
            down_part_copy(b).start()
        for copy in token_copies():
            copy.start()
        for copy in weight_copies(1):
            copy.start()

        def first_send(b, e):
            for step, flip in hops:
                first_copy(b, e, step, flip).start()

        def keep_own(e):
            for b in range(n_blocks):
                cols = columns(b)
                if BLOCKS[b][0] == 0:
                    recv_buf[e, source[0], :, :, cols] = send_buf[e, :, chip, core, :, cols]
                else:
                    recv_buf[e, source[1], :, :, cols] = send_buf[e, row, :, core, :, cols]

        def activation(gate_proj, up_proj):
            return (jax.nn.silu(gate_proj) * up_proj).astype(jnp.bfloat16)

        def down_step(e, slot, start, size, hidden):
            cols = pl.ds(start, size)
            y = jnp.dot(hidden, wd_buf[slot, :, cols], preferred_element_type=jnp.float32)
            send_buf[e, :, :, :, :, cols] = y.reshape(ring, ring, CORES, capacity, size).astype(jnp.bfloat16)

        gate_proj = up_proj = None
        for k in range(K_PARTS):
            for copy in part_copies(k):
                copy.wait()
            cols = k_slice(k)
            x_rows = x_buf[0, :, :, cols].reshape(rows, K_SIZES[k])
            gate_part = jnp.dot(x_rows, wg_buf[0, cols], preferred_element_type=jnp.float32)
            up_part = jnp.dot(x_rows, wu_buf[0, cols], preferred_element_type=jnp.float32)
            gate_proj = gate_part if gate_proj is None else gate_proj + gate_part
            up_proj = up_part if up_proj is None else up_proj + up_part
        hidden = activation(gate_proj, up_proj)
        for b in FIRST_ORDER:
            down_part_copy(b).wait()
            down_step(0, 0, BLOCKS[b][1], BLOCKS[b][2], hidden)
            if b == FIRST_ORDER[0]:
                pl.semaphore_wait(barrier, len(greet))
                for copy in weight_copies(2):
                    copy.start()
            first_send(b, 0)
        keep_own(0)

        for copy in token_copies():
            copy.wait()
        slots = slot_buf[...]
        keys = jnp.where(slots >= 0, eid_buf[...] * capacity + slots, -1).astype(jnp.float32)
        for h in range(HALVES):
            routes[h, 0, 0:top] = keys
            routes[h, 0, top:2 * top] = gate_buf[...]
        for h in range(HALVES):
            for step in range(1, ring):
                route_copy(h, step).start()

        @pl.loop(1, experts)
        def _(e):
            slot = lax.rem(e, WEIGHT_SLOTS)
            x_copy, gate_copy, up_copy, down_copy = weight_copies(e)
            x_copy.wait()
            x_rows = x_buf[slot].reshape(rows, width)
            gate_copy.wait()
            gate_proj = jnp.dot(x_rows, wg_buf[slot], preferred_element_type=jnp.float32)
            up_copy.wait()
            up_proj = jnp.dot(x_rows, wu_buf[slot], preferred_element_type=jnp.float32)
            hidden = activation(gate_proj, up_proj)
            down_copy.wait()

            @pl.when(e + 2 < experts)
            def _():
                for copy in weight_copies(e + 2):
                    copy.start()
            for part in reversed(range(DOWN_PARTS)):
                down_step(e, slot, part * down_size, down_size, hidden)
                for b in range(n_blocks // 2):
                    if (BLOCKS[b][1] + BLOCKS[b][2] - 1) // down_size == part:
                        first_send(b, e)

            @pl.when(e == experts - 1)
            def _():
                for b in FIRST_ORDER[n_blocks // 2:]:
                    first_send(b, e - 1)

            @pl.when(e != experts - 2)
            def _():
                for b in FIRST_ORDER[n_blocks // 2:]:
                    first_send(b, e)
            keep_own(e)

        route_all().wait_recv()
        line = lax.broadcasted_iota(jnp.int32, (part_rows, tokens), 0)
        local = line // (peers * capacity)
        src = lax.rem(line // capacity, peers)
        device = (row * peers + src, (src // CORES) * peers + chip * CORES + lax.rem(src, CORES))
        for h in range(HALVES):
            row_key = ((device[h] * experts + local) * capacity + lax.rem(line, capacity)).astype(jnp.float32)
            for step in range(ring):
                weight = jnp.zeros((part_rows, tokens), jnp.float32)
                for j in range(top):
                    weight = weight + jnp.where(row_key == routes[h, step, j:j + 1], routes[h, step, top + j:top + j + 1], 0.0)
                used_buf[h, step] = jnp.broadcast_to(jnp.max(weight, axis=1, keepdims=True), (part_rows, 128))
                weight = weight.T
                high = jnp.minimum(weight, BF16_MAX).astype(jnp.bfloat16)
                rest = weight - high.astype(jnp.float32)
                middle = rest.astype(jnp.bfloat16)
                low = (rest - middle.astype(jnp.float32)).astype(jnp.bfloat16)
                w_buf[h, step, 0:tokens] = high
                w_buf[h, step, tokens:2 * tokens] = middle
                w_buf[h, step, 2 * tokens:3 * tokens] = low

        def partial(b, step):
            h, _, size = BLOCKS[b]
            y = recv_buf[:, :, shift(place[h], step), :, columns(b)]
            y = y.astype(jnp.float32).reshape(part_rows, size)
            used = used_buf[h, step] > 0.0
            y = jnp.where(jnp.concatenate([used] * (size // 128), axis=1), y, 0.0).astype(jnp.bfloat16)
            part = jnp.dot(w_buf[h, step], y, preferred_element_type=jnp.float32)
            return part[0:tokens] + (part[tokens:2 * tokens] + part[2 * tokens:3 * tokens])

        late_core = core == 0
        for b in range(n_blocks):
            first_here(b).wait_recv()
            far = partial(b, 2)
            for way in range(2):
                far_out[way, :, columns(b)] = far[way * mid:(way + 1) * mid]
                far_copy(b, way).start()
            for way in range(2):
                near_out[way, :, columns(b)] = partial(b, near_step(way))

            @pl.when(jnp.logical_not(late_core))
            def _():
                for way in range(2):
                    own_copy(b, way).start()
            if b < n_blocks - 1:
                acc[:, columns(b)] = partial(b, 0)
        for b in range(n_blocks):
            for way in range(2):
                far_copy(b, way).wait_recv()
                part, cols = relay_part(way), columns(b)
                near_out[way, part, cols] = near_out[way, part, cols] + far_in[way, :, cols]
                sum_copy(b, way).start()
            if b == n_blocks - 1:
                acc[:, columns(b)] = partial(b, 0)
        for b in range(n_blocks):
            both_ways(b, sum_here).wait_recv()
            late = [n for trigger, n in LATE if trigger == b]
            if late:
                @pl.when(late_core)
                def _():
                    for n in late:
                        for way in range(2):
                            own_copy(n, way).start()
        for b in range(n_blocks):
            both_ways(b, own_here).wait_recv()
            cols = columns(b)
            out_ref[:, cols] = (acc[:, cols] + near_in[0, :, cols] + near_in[1, :, cols]).astype(jnp.bfloat16)

        route_all().wait_send()
        first_sent().wait_send()
        whole(far_out, far_sent.at[0], far_here.at[0, 0]).wait_send()
        whole(near_out, near_sent.at[0], own_here.at[0]).wait_send()

    return kernel


def solution(mesh):
    outer_devs = mesh.shape["outer"]
    inner_devs = mesh.shape["expert"]
    assert inner_devs == outer_devs * CORES and outer_devs == 4

    def local_step(x_disp, w_gate, w_up, w_down, slot_idx, expert_ids, gate_wts):
        group, experts, capacity, width = x_disp.shape
        ff = w_gate.shape[2]
        tokens, top = slot_idx.shape
        rows = group * capacity
        ring = outer_devs
        peers = inner_devs
        n_blocks = len(BLOCKS)
        bf16, f32 = jnp.bfloat16, jnp.float32
        hbm = pl.BlockSpec(memory_space=pltpu.HBM)
        dma = pltpu.SemaphoreType.DMA
        return pl.pallas_call(
            make_kernel(ring, experts, capacity, width, ff, tokens, top),
            out_shape=pltpu.VMEM((tokens, width), bf16),
            in_specs=[hbm] * 7,
            out_specs=pl.BlockSpec(memory_space=pltpu.VMEM),
            scratch_shapes=[
                pltpu.VMEM((WEIGHT_SLOTS, group, capacity, width), bf16),
                pltpu.VMEM((WEIGHT_SLOTS, width, ff), bf16),
                pltpu.VMEM((WEIGHT_SLOTS, width, ff), bf16),
                pltpu.VMEM((WEIGHT_SLOTS, ff, width), bf16),
                pltpu.VMEM((top, tokens), jnp.int32),
                pltpu.VMEM((top, tokens), jnp.int32),
                pltpu.VMEM((top, tokens), f32),
                pltpu.VMEM((experts, ring, ring, CORES, capacity, width), bf16),
                pltpu.VMEM((experts, peers, ring, capacity, width), bf16),
                pltpu.VMEM((HALVES, ring, 2 * top, tokens), f32),
                pltpu.VMEM((HALVES, ring, 3 * tokens, experts * peers * capacity), bf16),
                pltpu.VMEM((HALVES, ring, experts * peers * capacity, 128), f32),
                pltpu.VMEM((2, tokens // 2, width), f32),
                pltpu.VMEM((2, tokens // 2, width), f32),
                pltpu.VMEM((2, tokens, width), f32),
                pltpu.VMEM((2, tokens, width), f32),
                pltpu.VMEM((tokens, width), f32),
                dma((3, K_PARTS)),
                dma((n_blocks,)),
                dma((4, 2)),
                dma((3,)),
                dma((1,)),
                dma((n_blocks,)),
                dma((1,)),
                dma((1,)),
                dma((1,)),
                dma((n_blocks, 2)),
                dma((1,)),
                dma((n_blocks,)),
                dma((n_blocks,)),
            ],
            compiler_params=pltpu.CompilerParams(collective_id=0, has_side_effects=True, vmem_limit_bytes=VMEM_LIMIT),
        )(x_disp, w_gate, w_up, w_down, slot_idx.T, expert_ids.T, gate_wts.T)

    expert_spec = P(("outer", "expert"))
    token_spec = P(("data", "outer", "expert"))
    return jax.shard_map(local_step, mesh=mesh, in_specs=(P("data", ("outer", "expert")), expert_spec, expert_spec, expert_spec, token_spec, token_spec, token_spec), out_specs=token_spec, check_vma=False)
```

```python
import jax
import jax.numpy as jnp
from jax import lax
from jax.experimental import pallas as pl
from jax.experimental.pallas import tpu as pltpu
from jax.sharding import PartitionSpec as P

MESH_ID = pl.DeviceIdType.MESH
CORES = 2
BLOCKS = ((0, 0, 512), (1, 1024, 512), (0, 512, 512), (1, 1536, 512))
LATE = ((0, 0), (0, 1), (0, 2), (0, 3))
HALVES = 2
DOWN_PARTS = 2
K_SIZES = (512, 512, 512, 512)
K_PARTS = len(K_SIZES)
FIRST_ORDER = (1, 0, 3, 2)
WEIGHT_SLOTS = 3
VMEM_LIMIT = 62 * 2 ** 20
BF16_MAX = 3.3895313892515355e38


def make_kernel(ring, experts, capacity, width, ff, tokens, top):
    peers = ring * CORES
    group = ring * peers
    rows = group * capacity
    part_rows = experts * peers * capacity
    n_blocks = len(BLOCKS)
    down_size = width // DOWN_PARTS
    mid = tokens // 2

    def kernel(x_hbm, wg_hbm, wu_hbm, wd_hbm, slot_hbm, eid_hbm, gate_hbm, out_ref,
               x_buf, wg_buf, wu_buf, wd_buf, slot_buf, eid_buf, gate_buf, send_buf, recv_buf,
               routes, w_buf, used_buf, far_out, far_in, near_out, near_in, acc,
               part_sem, down_sem, weight_sem, token_sem, first_out, first_in, route_out, route_in,
               far_sent, far_here, near_sent, own_here, sum_here):
        row = lax.axis_index("outer")
        col = lax.axis_index("expert")
        chip, core = col // CORES, lax.rem(col, CORES)
        def columns(b):
            return pl.ds(BLOCKS[b][1], BLOCKS[b][2])

        place = (row, chip)
        source = (col, row * CORES + core)

        def shift(start, step):
            return lax.rem(start + step, ring)

        def ring_peer(h, step):
            if h == 0:
                return {"outer": shift(row, step), "expert": col}
            return {"outer": row, "expert": shift(chip, step) * CORES + core}

        def first_peer(h, step, flip):
            other = lax.rem(core + flip, CORES)
            if h == 0:
                to = shift(chip, step)
                return {"outer": row, "expert": to * CORES + other}, to, other
            to = shift(row, step)
            return {"outer": to, "expert": chip * CORES + other}, to, other

        def rows_for(h, e, to, other, cols):
            if h == 0:
                return send_buf.at[e, :, to, other, :, cols]
            return send_buf.at[e, to, :, other, :, cols]

        hops = [(2, 0), (2, 1), (1, 0), (ring - 1, 0), (1, 1), (ring - 1, 1), (0, 1)]

        def first_copy(b, e, step, flip):
            h = BLOCKS[b][0]
            peer, to, other = first_peer(h, step, flip)
            return pltpu.make_async_remote_copy(
                src_ref=rows_for(h, e, to, other, columns(b)),
                dst_ref=recv_buf.at[e, source[h], :, :, columns(b)],
                send_sem=first_out.at[0], recv_sem=first_in.at[b],
                device_id=peer, device_id_type=MESH_ID)

        def whole(ref, sent, here):
            return pltpu.make_async_remote_copy(
                src_ref=ref, dst_ref=ref, send_sem=sent, recv_sem=here,
                device_id=ring_peer(0, 1), device_id_type=MESH_ID)

        def first_here(b):
            return whole(recv_buf.at[:, pl.ds(0, peers - 1), :, :, columns(b)], first_out.at[0], first_in.at[b])

        def first_sent():
            return whole(recv_buf.at[:, pl.ds(0, peers - 1)], first_out.at[0], first_in.at[0])

        def route_copy(h, step):
            return pltpu.make_async_remote_copy(
                src_ref=routes.at[h, 0], dst_ref=routes.at[h, ring - step],
                send_sem=route_out.at[0], recv_sem=route_in.at[0],
                device_id=ring_peer(h, step), device_id_type=MESH_ID)

        def route_all():
            ref = routes.at[:, pl.ds(1, ring - 1)]
            return pltpu.make_async_remote_copy(
                src_ref=ref, dst_ref=ref, send_sem=route_out.at[0], recv_sem=route_in.at[0],
                device_id=ring_peer(0, 1), device_id_type=MESH_ID)

        def near_step(way):
            return 1 if way == 0 else ring - 1

        def relay_part(way):
            return pl.ds(way * mid, mid)

        def own_part(way):
            return pl.ds((1 - way) * mid, mid)

        def ring_copy(b, way, src, dst, sent, here):
            return pltpu.make_async_remote_copy(
                src_ref=src, dst_ref=dst, send_sem=sent.at[0], recv_sem=here,
                device_id=ring_peer(BLOCKS[b][0], near_step(way)), device_id_type=MESH_ID)

        def far_copy(b, way):
            cols = columns(b)
            return ring_copy(b, way, far_out.at[way, :, cols], far_in.at[way, :, cols], far_sent, far_here.at[b, way])

        def own_copy(b, way):
            cols, part = columns(b), own_part(way)
            return ring_copy(b, way, near_out.at[way, part, cols], near_in.at[way, part, cols], near_sent, own_here.at[b])

        def sum_copy(b, way):
            cols, part = columns(b), relay_part(way)
            return ring_copy(b, way, near_out.at[way, part, cols], near_in.at[way, part, cols], near_sent, sum_here.at[b])

        def both_ways(b, here):
            return whole(near_in.at[:, pl.ds(0, mid), columns(b)], near_sent.at[0], here.at[b])

        def k_slice(k):
            return pl.ds(sum(K_SIZES[:k]), K_SIZES[k])

        def part_copies(k):
            cols = k_slice(k)
            return (pltpu.make_async_copy(x_hbm.at[:, 0, :, cols], x_buf.at[0, :, :, cols], (weight_sem.at[0, 0] if k == 0 else part_sem.at[0, k - 1])),
                    pltpu.make_async_copy(wg_hbm.at[0, cols], wg_buf.at[0, cols], (weight_sem.at[1, 0] if k == 0 else part_sem.at[1, k - 1])),
                    pltpu.make_async_copy(wu_hbm.at[0, cols], wu_buf.at[0, cols], (weight_sem.at[2, 0] if k == 0 else part_sem.at[2, k - 1])))

        def down_part_copy(b):
            cols = columns(b)
            return pltpu.make_async_copy(wd_hbm.at[0, :, cols], wd_buf.at[0, :, cols], (weight_sem.at[3, 0] if b == FIRST_ORDER[0] else down_sem.at[b - int(b > FIRST_ORDER[0])]))

        def weight_copies(e):
            slot = lax.rem(e, WEIGHT_SLOTS)
            return (pltpu.make_async_copy(x_hbm.at[:, e], x_buf.at[slot], weight_sem.at[0, lax.rem(e, 2)]),
                    pltpu.make_async_copy(wg_hbm.at[e], wg_buf.at[slot], weight_sem.at[1, lax.rem(e, 2)]),
                    pltpu.make_async_copy(wu_hbm.at[e], wu_buf.at[slot], weight_sem.at[2, lax.rem(e, 2)]),
                    pltpu.make_async_copy(wd_hbm.at[e], wd_buf.at[slot], weight_sem.at[3, lax.rem(e, 2)]))

        def token_copies():
            return (pltpu.make_async_copy(slot_hbm, slot_buf, token_sem.at[0]),
                    pltpu.make_async_copy(eid_hbm, eid_buf, token_sem.at[1]),
                    pltpu.make_async_copy(gate_hbm, gate_buf, token_sem.at[2]))

        for k in range(K_PARTS):
            for copy in part_copies(k):
                copy.start()
        greet = [first_peer(h, step, flip)[0] for h in range(HALVES) for step, flip in hops[:-1]] + [first_peer(0, 0, 1)[0]]
        barrier = pltpu.get_barrier_semaphore()
        for peer in greet:
            pl.semaphore_signal(barrier, inc=1, device_id=peer, device_id_type=MESH_ID)
        for b in FIRST_ORDER:
            down_part_copy(b).start()
        for copy in token_copies():
            copy.start()
        for copy in weight_copies(1):
            copy.start()

        def first_send(b, e):
            for step, flip in hops:
                first_copy(b, e, step, flip).start()

        def keep_own(e):
            for b in range(n_blocks):
                cols = columns(b)
                if BLOCKS[b][0] == 0:
                    recv_buf[e, source[0], :, :, cols] = send_buf[e, :, chip, core, :, cols]
                else:
                    recv_buf[e, source[1], :, :, cols] = send_buf[e, row, :, core, :, cols]

        def activation(gate_proj, up_proj):
            return (jax.nn.silu(gate_proj) * up_proj).astype(jnp.bfloat16)

        def down_step(e, slot, start, size, hidden):
            cols = pl.ds(start, size)
            y = jnp.dot(hidden, wd_buf[slot, :, cols], preferred_element_type=jnp.float32)
            send_buf[e, :, :, :, :, cols] = y.reshape(ring, ring, CORES, capacity, size).astype(jnp.bfloat16)

        gate_proj = up_proj = None
        for k in range(K_PARTS):
            for copy in part_copies(k):
                copy.wait()
            cols = k_slice(k)
            x_rows = x_buf[0, :, :, cols].reshape(rows, K_SIZES[k])
            gate_part = jnp.dot(x_rows, wg_buf[0, cols], preferred_element_type=jnp.float32)
            up_part = jnp.dot(x_rows, wu_buf[0, cols], preferred_element_type=jnp.float32)
            gate_proj = gate_part if gate_proj is None else gate_proj + gate_part
            up_proj = up_part if up_proj is None else up_proj + up_part
        hidden = activation(gate_proj, up_proj)
        for b in FIRST_ORDER:
            down_part_copy(b).wait()
            down_step(0, 0, BLOCKS[b][1], BLOCKS[b][2], hidden)
            if b == FIRST_ORDER[0]:
                pl.semaphore_wait(barrier, len(greet))
                for copy in weight_copies(2):
                    copy.start()
            first_send(b, 0)
        keep_own(0)

        for copy in token_copies():
            copy.wait()
        slots = slot_buf[...]
        keys = jnp.where(slots >= 0, eid_buf[...] * capacity + slots, -1).astype(jnp.float32)
        for h in range(HALVES):
            routes[h, 0, 0:top] = keys
            routes[h, 0, top:2 * top] = gate_buf[...]
        for h in range(HALVES):
            for step in range(1, ring):
                route_copy(h, step).start()

        @pl.loop(1, experts)
        def _(e):
            slot = lax.rem(e, WEIGHT_SLOTS)
            x_copy, gate_copy, up_copy, down_copy = weight_copies(e)
            x_copy.wait()
            x_rows = x_buf[slot].reshape(rows, width)
            gate_copy.wait()
            gate_proj = jnp.dot(x_rows, wg_buf[slot], preferred_element_type=jnp.float32)
            up_copy.wait()
            up_proj = jnp.dot(x_rows, wu_buf[slot], preferred_element_type=jnp.float32)
            hidden = activation(gate_proj, up_proj)
            down_copy.wait()

            @pl.when(e + 2 < experts)
            def _():
                for copy in weight_copies(e + 2):
                    copy.start()
            for part in reversed(range(DOWN_PARTS)):
                down_step(e, slot, part * down_size, down_size, hidden)
                for b in range(n_blocks // 2):
                    if (BLOCKS[b][1] + BLOCKS[b][2] - 1) // down_size == part:
                        first_send(b, e)

            @pl.when(e == experts - 1)
            def _():
                for b in FIRST_ORDER[n_blocks // 2:]:
                    first_send(b, e - 1)

            @pl.when(e != experts - 2)
            def _():
                for b in FIRST_ORDER[n_blocks // 2:]:
                    first_send(b, e)
            keep_own(e)

        route_all().wait_recv()
        line = lax.broadcasted_iota(jnp.int32, (part_rows, tokens), 0)
        local = line // (peers * capacity)
        src = lax.rem(line // capacity, peers)
        device = (row * peers + src, (src // CORES) * peers + chip * CORES + lax.rem(src, CORES))
        for h in range(HALVES):
            row_key = ((device[h] * experts + local) * capacity + lax.rem(line, capacity)).astype(jnp.float32)
            for step in range(ring):
                weight = jnp.zeros((part_rows, tokens), jnp.float32)
                for j in range(top):
                    weight = weight + jnp.where(row_key == routes[h, step, j:j + 1], routes[h, step, top + j:top + j + 1], 0.0)
                used_buf[h, step] = jnp.broadcast_to(jnp.max(weight, axis=1, keepdims=True), (part_rows, 128))
                weight = weight.T
                high = jnp.minimum(weight, BF16_MAX).astype(jnp.bfloat16)
                rest = weight - high.astype(jnp.float32)
                middle = rest.astype(jnp.bfloat16)
                low = (rest - middle.astype(jnp.float32)).astype(jnp.bfloat16)
                w_buf[h, step, 0:tokens] = high
                w_buf[h, step, tokens:2 * tokens] = middle
                w_buf[h, step, 2 * tokens:3 * tokens] = low

        def partial(b, step):
            h, _, size = BLOCKS[b]
            y = recv_buf[:, :, shift(place[h], step), :, columns(b)]
            y = y.astype(jnp.float32).reshape(part_rows, size)
            used = used_buf[h, step] > 0.0
            y = jnp.where(jnp.concatenate([used] * (size // 128), axis=1), y, 0.0).astype(jnp.bfloat16)
            part = jnp.dot(w_buf[h, step], y, preferred_element_type=jnp.float32)
            return part[0:tokens] + (part[tokens:2 * tokens] + part[2 * tokens:3 * tokens])

        late_core = core == 0
        for b in range(n_blocks):
            first_here(b).wait_recv()
            far = partial(b, 2)
            for way in range(2):
                far_out[way, :, columns(b)] = far[way * mid:(way + 1) * mid]
                far_copy(b, way).start()
            for way in range(2):
                near_out[way, :, columns(b)] = partial(b, near_step(way))

            @pl.when(jnp.logical_not(late_core))
            def _():
                for way in range(2):
                    own_copy(b, way).start()
            if b < n_blocks - 1:
                acc[:, columns(b)] = partial(b, 0)
        for b in range(n_blocks):
            for way in range(2):
                far_copy(b, way).wait_recv()
                part, cols = relay_part(way), columns(b)
                near_out[way, part, cols] = near_out[way, part, cols] + far_in[way, :, cols]
                sum_copy(b, way).start()
            if b == n_blocks - 1:
                acc[:, columns(b)] = partial(b, 0)
        for b in range(n_blocks):
            both_ways(b, sum_here).wait_recv()
            late = [n for trigger, n in LATE if trigger == b]
            if late:
                @pl.when(late_core)
                def _():
                    for n in late:
                        for way in range(2):
                            own_copy(n, way).start()
        for b in range(n_blocks):
            both_ways(b, own_here).wait_recv()
            cols = columns(b)
            out_ref[:, cols] = (acc[:, cols] + near_in[0, :, cols] + near_in[1, :, cols]).astype(jnp.bfloat16)

        route_all().wait_send()
        first_sent().wait_send()
        whole(far_out, far_sent.at[0], far_here.at[0, 0]).wait_send()
        whole(near_out, near_sent.at[0], own_here.at[0]).wait_send()

    return kernel


def solution(mesh):
    outer_devs = mesh.shape["outer"]
    inner_devs = mesh.shape["expert"]
    assert inner_devs == outer_devs * CORES and outer_devs == 4

    def local_step(x_disp, w_gate, w_up, w_down, slot_idx, expert_ids, gate_wts):
        group, experts, capacity, width = x_disp.shape
        ff = w_gate.shape[2]
        tokens, top = slot_idx.shape
        rows = group * capacity
        ring = outer_devs
        peers = inner_devs
        n_blocks = len(BLOCKS)
        bf16, f32 = jnp.bfloat16, jnp.float32
        hbm = pl.BlockSpec(memory_space=pltpu.HBM)
        dma = pltpu.SemaphoreType.DMA
        return pl.pallas_call(
            make_kernel(ring, experts, capacity, width, ff, tokens, top),
            out_shape=pltpu.VMEM((tokens, width), bf16),
            in_specs=[hbm] * 7,
            out_specs=pl.BlockSpec(memory_space=pltpu.VMEM),
            scratch_shapes=[
                pltpu.VMEM((WEIGHT_SLOTS, group, capacity, width), bf16),
                pltpu.VMEM((WEIGHT_SLOTS, width, ff), bf16),
                pltpu.VMEM((WEIGHT_SLOTS, width, ff), bf16),
                pltpu.VMEM((WEIGHT_SLOTS, ff, width), bf16),
                pltpu.VMEM((top, tokens), jnp.int32),
                pltpu.VMEM((top, tokens), jnp.int32),
                pltpu.VMEM((top, tokens), f32),
                pltpu.VMEM((experts, ring, ring, CORES, capacity, width), bf16),
                pltpu.VMEM((experts, peers, ring, capacity, width), bf16),
                pltpu.VMEM((HALVES, ring, 2 * top, tokens), f32),
                pltpu.VMEM((HALVES, ring, 3 * tokens, experts * peers * capacity), bf16),
                pltpu.VMEM((HALVES, ring, experts * peers * capacity, 128), f32),
                pltpu.VMEM((2, tokens // 2, width), f32),
                pltpu.VMEM((2, tokens // 2, width), f32),
                pltpu.VMEM((2, tokens, width), f32),
                pltpu.VMEM((2, tokens, width), f32),
                pltpu.VMEM((tokens, width), f32),
                dma((3, K_PARTS - 1)),
                dma((n_blocks - 1,)),
                dma((4, 2)),
                dma((3,)),
                dma((1,)),
                dma((n_blocks,)),
                dma((1,)),
                dma((1,)),
                dma((1,)),
                dma((n_blocks, 2)),
                dma((1,)),
                dma((n_blocks,)),
                dma((n_blocks,)),
            ],
            compiler_params=pltpu.CompilerParams(collective_id=0, has_side_effects=True, vmem_limit_bytes=VMEM_LIMIT),
        )(x_disp, w_gate, w_up, w_down, slot_idx.T, expert_ids.T, gate_wts.T)

    expert_spec = P(("outer", "expert"))
    token_spec = P(("data", "outer", "expert"))
    return jax.shard_map(local_step, mesh=mesh, in_specs=(P("data", ("outer", "expert")), expert_spec, expert_spec, expert_spec, token_spec, token_spec, token_spec), out_specs=token_spec, check_vma=False)
```
